32 devices in a mesh: seq: 8 (over z, x), dp: 4 (over y, core).
Axes of the slice: x: 2, y: 2, z: 4, core: 2. Of those that a mesh axis runs over, the one named last changes fastest.
Arguments:
- conv_input: bfloat16 [4, 2048, 2816], P('dp', 'seq'), may hold values from -6 to 6
- gate_input: bfloat16 [4, 2048, 2560], P('dp', 'seq'), may hold values from -6 to 6
- step_input: float32 [4, 40, 2048], P('dp', None, 'seq'), may hold values from -7.5 to 2048
- filter_taps: float32 [4, 2816], replicated, may hold values from -3 to 3
- filter_bias: float32 [2816], replicated, may hold values from -0.5 to 0.5
- step_bias: float32 [40], replicated, may hold values from -1 to 1
- decay_log: float32 [40], replicated, may hold values from -13 to 3
- skip_gain: float32 [40], replicated, may hold values from 0.5 to 1.5
- norm_weight: float32 [2560], replicated, may hold values from 0.5 to 1.5
- output_weight: bfloat16 [2560, 1280], P('dp'), may hold values from -0.125 to 0.125
- output_grad: bfloat16 [4, 2048, 1280], P('dp', 'seq'), may hold values from -6 to 6
Outputs:
- input_grad: bfloat16 [4, 2048, 2816], P('dp', 'seq')
- gate_grad: bfloat16 [4, 2048, 2560], P('dp', 'seq')
- step_grad: float32 [4, 40, 2048], P('dp', None, 'seq')
- weight_grad: float32 [2560, 1280], P('dp')
- filter_grads: float32 [5, 2816], replicated
- norm_grad: float32 [2560], replicated
- head_grads: float32 [3, 40], replicated
The draws below stay inside these ranges and needn't reach their ends.
All inputs are finite; a program needn't handle non-finite values.
Results may differ from the reference program's by a relative error of at most 0.0029.
Values may be sent and summed in bfloat16 or wider, within the bound.
A program may use at most 192 MiB of HBM per device.

```python
import jax
import jax.numpy as jnp
from jax import lax

HEADS = 40
HEAD_DIM = 64
STATE = 128
WIDTH = 1280
SPAN = 256
KERNEL = 4
TOKENS_DEV = 256
INNER = 2560
CHANNELS = 2816
SEQ_LEN = 2048
BATCH = 4


def head_rates(key):
    folded = jax.random.fold_in(key, 4099)
    slow_key, fast_key, pick_key = jax.random.split(folded, 3)
    slow_rate = jax.random.uniform(slow_key, (HEADS,), jnp.float32, 10.0, 30.0) / (0.03 * SEQ_LEN)
    fast_rate = 1.0 / (0.03 * jax.random.uniform(fast_key, (HEADS,), jnp.float32, 30.0, 50.0))
    share = 0.5
    chosen = jax.random.uniform(pick_key, (HEADS,), jnp.float32) < share
    return jnp.where(chosen, fast_rate, slow_rate)


def draw_decay_log(key, part):
    return jnp.log(head_rates(key))


def draw_step_input(key, part):
    rates = head_rates(key)
    folded = jax.random.fold_in(key, 8191)
    noise_key, block_key, place_key, loss_key = jax.random.split(folded, 4)
    noise = jax.random.uniform(noise_key, (BATCH, HEADS, SEQ_LEN), jnp.float32, -5.5, -2.5)
    levels = jax.random.uniform(block_key, (BATCH, HEADS, SEQ_LEN // TOKENS_DEV, 1), jnp.float32, -1.0, 1.0)
    spread = jnp.broadcast_to(levels, (BATCH, HEADS, SEQ_LEN // TOKENS_DEV, TOKENS_DEV)).reshape(BATCH, HEADS, SEQ_LEN)
    places = jax.random.randint(place_key, (BATCH, 2), 0, SEQ_LEN)
    marked = jnp.any(jnp.arange(SEQ_LEN)[None, None, :] == places[:, :, None], axis=1)
    losses = jax.random.uniform(loss_key, (BATCH, HEADS, 1), jnp.float32, 0.2, 0.45)
    jumps = -jnp.log(1.0 - losses) / rates[None, :, None]
    return jnp.where(marked[:, None, :], jumps, noise + spread)


def block_levels(rng, extent, cuts, least, high):
    loudness = 1.0
    for dim, parts in cuts:
        draws = jax.random.uniform(jax.random.fold_in(jax.random.fold_in(rng, 6), dim), (parts,), jnp.float32, least / len(cuts), high / len(cuts))
        loudness = loudness * jnp.repeat(jnp.exp(draws), extent[dim] // parts).reshape((-1,) + (1,) * (len(extent) - 1 - dim))
    return loudness


def scatter_about(stream_key, shape, scale, limit, cuts=(), kind=jnp.bfloat16):
    loudness = block_levels(stream_key, shape, cuts, -0.22, 0.18) if cuts else 1.0
    values = jax.random.normal(stream_key, shape, jnp.float32) * scale * loudness
    return jnp.minimum(jnp.maximum(values, -limit), limit).astype(kind)


def setup_inputs(seed: int = 0) -> dict:
    streams_of = jax.random.split(jax.random.key(seed), 12)
    return {
        "conv_input": scatter_about(streams_of[0], (BATCH, SEQ_LEN, CHANNELS), 1.0, 6.0, ((0, 4), (1, 8))),
        "gate_input": scatter_about(streams_of[1], (BATCH, SEQ_LEN, INNER), 1.0, 6.0, ((0, 4), (1, 8))),
        "step_input": draw_step_input(jax.random.fold_in(streams_of[11], 71), 0),
        "filter_taps": scatter_about(streams_of[3], (KERNEL, CHANNELS), KERNEL ** -0.5, 3.0, (), jnp.float32),
        "filter_bias": jnp.clip(jax.random.uniform(streams_of[4], (CHANNELS,), jnp.float32, -0.5, 0.5), -0.5, 0.5),
        "step_bias": jnp.clip(jax.random.uniform(streams_of[5], (HEADS,), jnp.float32, -1.0, 1.0), -1.0, 1.0),
        "decay_log": draw_decay_log(jax.random.fold_in(streams_of[11], 71), 0),
        "skip_gain": jnp.clip(jax.random.uniform(streams_of[7], (HEADS,), jnp.float32, 0.5, 1.5), 0.5, 1.5),
        "norm_weight": jnp.clip(1.0 + 0.1 * jax.random.normal(streams_of[8], (INNER,), jnp.float32), 0.5, 1.5),
        "output_weight": scatter_about(streams_of[9], (INNER, WIDTH), INNER ** -0.5, 0.125, ((0, 4),)),
        "output_grad": scatter_about(streams_of[10], (BATCH, SEQ_LEN, WIDTH), 1.0, 6.0, ((0, 4), (1, 8))),
    }


HIGHEST = lax.Precision.HIGHEST
MASKED = -1e+30
EPSILON = 1e-05

def block_step(skip_gain, carried, slices):
    activated, block_steps, block_rates = slices
    length = activated.shape[0]
    values = activated[:, :INNER].reshape(length, HEADS, HEAD_DIM)
    key_side = activated[:, INNER:INNER + STATE]
    query_side = activated[:, INNER + STATE:]
    cumsums = jnp.cumsum(block_rates, axis=1)
    scaled = values * block_steps.T[:, :, None]
    to_end = jnp.exp(cumsums[:, -1:] - cumsums)
    block_state = jnp.einsum('hs,shp,sn->hpn', to_end, scaled, key_side, precision=HIGHEST)
    scores = jnp.einsum('tn,sn->ts', query_side, key_side, precision=HIGHEST)
    differences = cumsums[:, :, None] - cumsums[:, None, :]
    causal = jnp.tril(jnp.ones((length, length), dtype=bool))
    weights = scores[None] * jnp.exp(jnp.where(causal[None], differences, MASKED))
    inside = jnp.einsum('hts,shp->thp', weights, scaled, precision=HIGHEST)
    from_state = jnp.einsum('tn,hpn->thp', query_side, carried, precision=HIGHEST) * jnp.exp(cumsums).T[:, :, None]
    result = inside + from_state + skip_gain[:, None] * values
    updated = jnp.exp(cumsums[:, -1])[:, None, None] * carried + block_state
    return (updated, result.reshape(length, INNER))

def layer_forward(raw_rows, gate_rows, step_rows, filter_taps, filter_bias, step_bias, decay_log, skip_gain, norm_weight):
    length = raw_rows.shape[0]
    padded = jnp.concatenate([jnp.zeros((KERNEL - 1, CHANNELS), jnp.float32), raw_rows], axis=0)
    filtered = filter_bias + filter_taps[0] * padded[0:length]
    for offset in range(1, KERNEL):
        filtered = filtered + filter_taps[offset] * padded[offset:offset + length]
    activated = jax.nn.silu(filtered)
    step_sizes = jax.nn.softplus(step_rows + step_bias[:, None])
    decay_rates = step_sizes * (-jnp.exp(decay_log))[:, None]
    blocks = length // SPAN
    pieces = (activated.reshape(blocks, SPAN, CHANNELS), step_sizes.reshape(HEADS, blocks, SPAN).transpose(1, 0, 2), decay_rates.reshape(HEADS, blocks, SPAN).transpose(1, 0, 2))
    stepper = jax.checkpoint(lambda carried, slices: block_step(skip_gain, carried, slices))
    _, outputs = lax.scan(stepper, jnp.zeros((HEADS, HEAD_DIM, STATE), jnp.float32), pieces)
    scanned = outputs.reshape(length, INNER)
    gated = scanned * jax.nn.silu(gate_rows)
    inverse_rms = lax.rsqrt(lax.optimization_barrier(jnp.mean(gated * gated, axis=1, keepdims=True)) + EPSILON)
    return gated * inverse_rms * norm_weight

def reference(conv_input, gate_input, step_input, filter_taps, filter_bias, step_bias, decay_log, skip_gain, norm_weight, output_weight, output_grad):

    def one_sequence(slices):
        raw_rows, gate_rows, step_rows, cotangent = slices
        normed, pullback = jax.vjp(layer_forward, raw_rows.astype(jnp.float32), gate_rows.astype(jnp.float32), step_rows, filter_taps, filter_bias, step_bias, decay_log, skip_gain, norm_weight)
        normed_low = normed.astype(jnp.bfloat16)
        normed_grad = jnp.dot(cotangent, output_weight.T, preferred_element_type=jnp.float32)
        weight_term = jnp.dot(normed_low.T, cotangent, preferred_element_type=jnp.float32)
        return tuple(pullback(normed_grad)) + (weight_term,)
    results = lax.map(one_sequence, (conv_input, gate_input, step_input, output_grad))
    input_grad = results[0].astype(jnp.bfloat16)
    gate_grad = results[1].astype(jnp.bfloat16)
    step_grad = results[2]
    filter_grads = jnp.concatenate([lax.optimization_barrier(jnp.sum(results[3], axis=0)), lax.optimization_barrier(jnp.sum(results[4], axis=0))[None]], axis=0)
    head_grads = jnp.stack([lax.optimization_barrier(jnp.sum(results[5], axis=0)), lax.optimization_barrier(jnp.sum(results[6], axis=0)), lax.optimization_barrier(jnp.sum(results[7], axis=0))])
    norm_grad = lax.optimization_barrier(jnp.sum(results[8], axis=0))
    weight_grad = lax.optimization_barrier(jnp.sum(results[9], axis=0))
    return (input_grad, gate_grad, step_grad, weight_grad, filter_grads, norm_grad, head_grads)
```

```python
import functools

import jax
import jax.numpy as jnp
from jax import lax
from jax.experimental import pallas as pl
from jax.experimental.pallas import tpu as pltpu
from jax.sharding import PartitionSpec as P

F32 = jnp.float32
BF16 = jnp.bfloat16
EPSILON = 1e-05
LOG2E = 1.4426950408889634
LANES = 128
HEAD_DIM = 64
GROUP = 2
MESH = pl.DeviceIdType.MESH
NN = (((1,), (0,)), ((), ()))
NT = (((1,), (1,)), ((), ()))
TN = (((0,), (0,)), ((), ()))


def dot(a, b, dims=NN):
    return lax.dot_general(a, b, dims, preferred_element_type=F32)


def rounded_high(a):
    scaled = a * 65537.0
    return scaled - (scaled - a)


def split2(a):
    high = rounded_high(a)
    return high.astype(BF16), (a - high).astype(BF16)


def split3(a):
    high = rounded_high(a)
    rest = a - high
    middle = rounded_high(rest)
    return high.astype(BF16), middle.astype(BF16), (rest - middle).astype(BF16)


def dot3(a, b, dims=NN):
    return dot(a[0], b[0], dims) + (dot(a[0], b[1], dims) + dot(a[1], b[0], dims))


def chunk_of(index):
    return pl.ds(pl.multiple_of(index * LANES, LANES), LANES)


def iota(shape, dim):
    return lax.broadcasted_iota(jnp.int32, shape, dim)


def low_half(shape):
    return iota(shape, 1) < HEAD_DIM


def head_rows(index):
    shape = (LANES, LANES)
    wanted = 2 * index + jnp.where(low_half(shape), 0, 1)
    return jnp.where(iota(shape, 0) == wanted, 1.0, 0.0).astype(BF16)


def sigmoid(a):
    return 1.0 / (1.0 + jnp.exp(-a))


def transposed(rows):
    heads, tokens = rows.shape
    padded = jnp.concatenate([rows, jnp.zeros((LANES - heads, tokens), F32)], axis=0)
    return padded.T


def step_phase(step, step_bias, decay_log, cum_rows, cum_cols, dt_cols):
    shifted = step[...] + step_bias[...]
    sizes = jnp.maximum(shifted, 0.0) + jnp.log1p(jnp.exp(-jnp.abs(shifted)))
    rates = -jnp.exp(decay_log[...]) * sizes
    tokens = rates.shape[1]
    shape = (tokens, tokens)
    before = jnp.where(iota(shape, 0) <= iota(shape, 1), 1.0, 0.0).astype(BF16)
    high, middle, low = split3(rates)
    cumulative = (dot(high, before) + (dot(middle, before) + dot(low, before))) * LOG2E
    for head in range(rates.shape[0]):
        cum_rows[head] = cumulative[head : head + 1]
    cum_cols[...] = transposed(cumulative)
    dt_cols[...] = transposed(sizes)


def expand_phase(cum_cols, dt_cols, cum_wide, dt_wide, decay_wide):
    tokens, inner = cum_wide.shape
    cum_parts = split3(cum_cols[...])
    dt_parts = split3(dt_cols[...])

    def each(index, carry):
        here = chunk_of(index)
        rows = head_rows(index)
        wide = dot(cum_parts[0], rows) + (dot(cum_parts[1], rows) + dot(cum_parts[2], rows))
        cum_wide[:, here] = wide
        dt_wide[:, here] = dot(dt_parts[0], rows) + (
            dot(dt_parts[1], rows) + dot(dt_parts[2], rows)
        )
        decay_wide[:, here] = jnp.broadcast_to(jnp.exp2(wide[tokens - 1 : tokens]), (8, LANES))
        return carry

    lax.fori_loop(0, inner // LANES, each, 0)


def filter_chunk(here, raw, halo, taps, bias, window, act, slope):
    tokens = raw.shape[0]
    window[0:8, :] = halo[:, here].astype(F32)[8:]
    window[8 : 8 + tokens, :] = raw[:, here].astype(F32)
    count = taps.shape[0]
    filtered = bias[:, here] + taps[0:1, here] * window[9 - count : 9 - count + tokens, :]
    for k in range(1, count):
        filtered = filtered + taps[k : k + 1, here] * window[9 - count + k : 9 - count + k + tokens, :]
    gate = sigmoid(filtered)
    result = filtered * gate
    act[:, here] = result
    slope[:, here] = gate + result * (1.0 - gate)
    return result


def in_messages(total, after, each, carry):
    def several(message, carry):
        for j in range(GROUP):
            carry = each(message * GROUP + j, carry)
        after(message)
        return carry

    return lax.fori_loop(0, total // GROUP, several, carry)


def state_phase(
    raw, halo, taps, bias, window, act, slope, cum_wide, dt_wide, key_t, query_t, states, after
):
    tokens, inner = cum_wide.shape
    first = inner // LANES
    key = filter_chunk(pl.ds(inner, LANES), raw, halo, taps, bias, window, act, slope)
    query = filter_chunk(pl.ds(inner + LANES, LANES), raw, halo, taps, bias, window, act, slope)
    high, low = split2(key.T)
    key_t[0], key_t[1] = high, low
    high, low = split2(query.T)
    query_t[0], query_t[1] = high, low

    def each(index, carry):
        here = chunk_of(index)
        values = filter_chunk(here, raw, halo, taps, bias, window, act, slope)
        cum = cum_wide[:, here]
        moved = values * dt_wide[:, here] * jnp.exp2(cum[tokens - 1 : tokens] - cum)
        states[index] = dot3((key_t[0], key_t[1]), split2(moved))
        return carry

    in_messages(first, after, each, 0)


def score_blocks(act, inner, scores):
    half = act.shape[0] // 2
    key = split2(act[:, inner : inner + LANES])
    query = split2(act[:, inner + LANES : inner + 2 * LANES])
    shape = (half, half)
    causal = iota(shape, 0) >= iota(shape, 1)
    for slot, (rows, columns) in enumerate(((0, 0), (1, 1), (1, 0))):
        left = tuple(part[rows * half : (rows + 1) * half] for part in query)
        right = tuple(part[columns * half : (columns + 1) * half] for part in key)
        block = dot3(left, right, NT)
        if rows == columns:
            block = jnp.where(causal, block, 0.0)
        scores[slot] = block


def decay_blocks(index, cum, cum_rows, half, block):
    rows = slice(block * half, (block + 1) * half)
    found = []
    for j in range(2):
        column = jnp.broadcast_to(cum[rows, j * HEAD_DIM : j * HEAD_DIM + 1], (half, half))
        row = cum_rows[2 * index + j][:, rows]
        found.append(jnp.exp2(jnp.minimum(column - row, 0.0)))
    return jnp.concatenate(found, axis=1)


def stacked(block):
    low = low_half(block.shape)
    zero = jnp.zeros_like(block)
    return jnp.concatenate([jnp.where(low, block, zero), jnp.where(low, zero, block)], axis=0)


def inside_phase(act, cum_wide, dt_wide, cum_rows, scores, inside, after):
    tokens, inner = cum_wide.shape
    half = tokens // 2

    def each(index, carry):
        here = chunk_of(index)
        scaled = act[:, here] * dt_wide[:, here]
        cum = cum_wide[:, here]
        for block in range(2):
            rows = slice(block * half, (block + 1) * half)
            weights = decay_blocks(index, cum, cum_rows, half, block)
            score = scores[block]
            weights = jnp.concatenate([score, score], axis=1) * weights
            right = stacked(scaled[rows])
            result = dot3(split2(weights), split2(right))
            if block == 1:
                middle = cum[half - 1 : half]
                moved = scaled[:half] * jnp.exp2(middle - cum[:half])
                result = result + jnp.exp2(cum[half:] - middle) * dot3(
                    split2(scores[2]), split2(moved)
                )
            inside[rows, here] = result
        return carry

    in_messages(inner // LANES, after, each, 0)


def norm_phase(act, cum_wide, inside, entering, skip_wide, gate, norm_weight, gated, scale, low):
    tokens, inner = cum_wide.shape
    query = split2(act[:, inner + LANES : inner + 2 * LANES])

    def each(index, total):
        here = chunk_of(index)
        crossed = jnp.exp2(cum_wide[:, here]) * dot3(query, split2(entering[index]))
        scanned = inside[:, here] + crossed
        inside[:, here] = scanned
        scanned = scanned + skip_wide[:, here] * act[:, here]
        branch = gate[:, here].astype(F32)
        result = scanned * (branch * sigmoid(branch))
        gated[:, here] = result
        return total + result * result

    total = lax.fori_loop(0, inner // LANES, each, jnp.zeros((tokens, LANES), F32))
    mean = jnp.sum(total, axis=1, keepdims=True) / inner
    inverse = lax.rsqrt(mean + EPSILON)
    scale[...] = jnp.broadcast_to(inverse, scale.shape)

    per = low.shape[2] // LANES

    def rounded(index, carry):
        here = chunk_of(index)
        place = pl.ds(pl.multiple_of(index % per * LANES, LANES), LANES)
        result = gated[:, here] * scale[...] * norm_weight[:, here]
        low[index // per, :, place] = result.astype(BF16)
        return carry

    lax.fori_loop(0, inner // LANES, rounded, 0)


def gate_phase(
    act, cum_wide, inside, skip_wide, gate, norm_weight, gated, scale, query_t, cotangent, weight,
    normed_grad, scanned_grad, gate_grad, norm_grad, skip_sum, entering_grad,
    after,
):
    tokens, inner = cum_wide.shape
    own = cotangent[...]

    def first(index, total):
        here = chunk_of(index)
        rows = weight[pl.ds(pl.multiple_of(index * LANES, LANES), LANES), :]
        found = dot(own, rows, NT)
        normed_grad[:, here] = found
        return total + found * norm_weight[:, here] * gated[:, here]

    total = lax.fori_loop(0, inner // LANES, first, jnp.zeros((tokens, LANES), F32))
    inverse = scale[...]
    pull = jnp.sum(total, axis=1, keepdims=True) / inner * inverse * inverse * inverse

    def second(index, carry):
        here = chunk_of(index)
        found = normed_grad[:, here]
        product = gated[:, here]
        norm_grad[:, here] = jnp.broadcast_to(
            jnp.sum(found * product * inverse, axis=0, keepdims=True), (8, LANES)
        )
        down = inverse * (found * norm_weight[:, here]) - product * pull
        branch = gate[:, here].astype(F32)
        opened = sigmoid(branch)
        passed = branch * opened
        values = act[:, here]
        scanned = inside[:, here] + skip_wide[:, here] * values
        gate_grad[:, here] = (down * scanned * (opened + passed * (1.0 - opened))).astype(BF16)
        back = down * passed
        scanned_grad[:, here] = back
        skip_sum[:, here] = jnp.broadcast_to(
            jnp.sum(back * values, axis=0, keepdims=True), (8, LANES)
        )
        moved = back * jnp.exp2(cum_wide[:, here])
        entering_grad[index] = dot3((query_t[0], query_t[1]), split2(moved))
        return carry

    in_messages(inner // LANES, after, second, 0)


def inside_grad_phase(
    act, cum_wide, dt_wide, cum_rows, scores, inside, scanned_grad, entering,
    scaled_grad, score_grad, query_grad, row_sums, after,
):
    tokens, inner = cum_wide.shape
    half = tokens // 2
    score_grad[...] = jnp.zeros_like(score_grad)
    query_grad[...] = jnp.zeros_like(query_grad)
    row_sums[...] = jnp.zeros_like(row_sums)

    def each(index, carry):
        here = chunk_of(index)
        scaled = act[:, here] * dt_wide[:, here]
        cum = cum_wide[:, here]
        back = scanned_grad[:, here]
        middle = cum[half - 1 : half]
        for block in range(2):
            rows = slice(block * half, (block + 1) * half)
            decay = decay_blocks(index, cum, cum_rows, half, block)
            score = scores[block]
            weights = split2(jnp.concatenate([score, score], axis=1) * decay)
            down = split2(back[rows])
            products = dot3(down, split2(stacked(scaled[rows])), NT) * decay
            score_grad[block] += products[:, :half] + products[:, half:]
            found = dot3(weights, down, TN)
            found = jnp.where(low_half((half, LANES)), found[:half], found[half:])
            if block == 0:
                pulled = split2(back[half:] * jnp.exp2(cum[half:] - middle))
                factor = jnp.exp2(middle - cum[:half])
                score_grad[2] += dot3(pulled, split2(scaled[:half] * factor), NT)
                found = found + factor * dot3(split2(scores[2]), pulled, TN)
            scaled_grad[rows, here] = found
        query_grad[...] += dot3(split2(back * jnp.exp2(cum)), split2(entering[index]), NT)
        rows = head_rows(index)
        high, low = split2(back * inside[:, here])
        row_sums[...] += dot(high, rows, NT) + dot(low, rows, NT)
        return carry

    in_messages(inner // LANES, after, each, 0)


def end_phase(
    act, slope, cum_wide, dt_wide, cum_cols, dt_cols, decay_wide, skip_wide, scanned_grad,
    scaled_grad, score_grad, query_grad, row_sums, entering, end_grad, key_grad, skip_sum,
    step, step_bias, decay_row, raw, halo, taps, window, filtered_grad,
    step_grad, filter_sums, head_sums,
):
    tokens, inner = cum_wide.shape
    half = tokens // 2
    key = split2(act[:, inner : inner + LANES])
    query = split2(act[:, inner + LANES : inner + 2 * LANES])
    count = taps.shape[0]

    def finish(here, found):
        pulled = found * slope[:, here]
        filtered_grad[:, here] = pulled
        window[0:8, :] = halo[:, here].astype(F32)[8:]
        window[8 : 8 + tokens, :] = raw[:, here].astype(F32)
        sums = [
            jnp.sum(pulled * window[9 - count + k : 9 - count + k + tokens, :], axis=0, keepdims=True)
            for k in range(count)
        ]
        sums.append(jnp.sum(pulled, axis=0, keepdims=True))
        sums.append(jnp.zeros((8 - len(sums), LANES), F32))
        filter_sums[:, here] = jnp.concatenate(sums, axis=0)

    key_grad[...] = jnp.zeros_like(key_grad)
    zeros = (jnp.zeros((tokens, LANES), F32), jnp.zeros((8, LANES), F32), jnp.zeros((8, LANES), F32))

    def each(index, sums):
        value_sums, last_sums, skip_sums = sums
        here = chunk_of(index)
        values = act[:, here]
        sizes = dt_wide[:, here]
        cum = cum_wide[:, here]
        to_end = jnp.exp2(cum[tokens - 1 : tokens] - cum)
        after = end_grad[index]
        parts = split2(after)
        moved = values * sizes * to_end
        moved_grad = dot3(key, parts)
        key_grad[...] += dot3(split2(moved), parts, NT)
        last = jnp.sum(moved * moved_grad, axis=0, keepdims=True) + decay_wide[0:1, here] * jnp.sum(
            after * entering[index], axis=0, keepdims=True
        )
        scaled = scaled_grad[:, here] + to_end * moved_grad
        rows = head_rows(index)
        high, low = split2(scaled * values)
        value_sums = value_sums + (dot(high, rows, NT) + dot(low, rows, NT))
        parts = split3(jnp.broadcast_to(last, (8, LANES)))
        last_sums = last_sums + (dot(parts[0], rows, NT) + (dot(parts[1], rows, NT) + dot(parts[2], rows, NT)))
        parts = split3(skip_sum[:, here])
        skip_sums = skip_sums + (dot(parts[0], rows, NT) + (dot(parts[1], rows, NT) + dot(parts[2], rows, NT)))
        finish(here, scaled * sizes + skip_wide[:, here] * scanned_grad[:, here])
        return value_sums, last_sums, skip_sums

    value_sums, last_sums, skip_sums = lax.fori_loop(0, inner // LANES, each, zeros)

    shape = (half, half)
    causal = iota(shape, 0) >= iota(shape, 1)
    blocks = [split2(jnp.where(causal, score_grad[slot], 0.0)) for slot in range(2)]
    blocks.append(split2(score_grad[2]))
    first = lambda parts: tuple(part[:half] for part in parts)
    second = lambda parts: tuple(part[half:] for part in parts)
    upper = dot3(blocks[0], first(key))
    lower = dot3(blocks[1], second(key)) + dot3(blocks[2], first(key))
    finish(pl.ds(inner + LANES, LANES), query_grad[...] + jnp.concatenate([upper, lower], axis=0))
    upper = dot3(blocks[0], first(query), TN) + dot3(blocks[2], second(query), TN)
    lower = dot3(blocks[1], second(query), TN)
    finish(pl.ds(inner, LANES), key_grad[...] + jnp.concatenate([upper, lower], axis=0))

    sizes = dt_cols[...]
    cum_grad = row_sums[...] - sizes * value_sums
    at_end = iota((tokens, LANES), 0) == tokens - 1
    cum_grad = cum_grad + jnp.where(at_end, jnp.broadcast_to(last_sums[0:1], (tokens, LANES)), 0.0)
    shape = (tokens, tokens)
    after = jnp.where(iota(shape, 0) <= iota(shape, 1), 1.0, 0.0).astype(BF16)
    parts = split3(cum_grad)
    rate_grad = dot(after, parts[0]) + (dot(after, parts[1]) + dot(after, parts[2]))
    rate = -jnp.exp(decay_row[...])
    heads = step.shape[0]
    shifted = transposed(step[...] + step_bias[...])
    pulled = (value_sums + rate_grad * rate) * sigmoid(shifted)
    pulled = jnp.where(iota((tokens, LANES), 1) < heads, pulled, 0.0)
    step_grad[...] = pulled.T[:heads]
    head_sums[...] = jnp.concatenate(
        [
            jnp.sum(pulled, axis=0, keepdims=True),
            jnp.sum(rate_grad * rate * sizes, axis=0, keepdims=True),
            skip_sums[0:1],
            jnp.zeros((5, LANES), F32),
        ],
        axis=0,
    )


def filter_grad_phase(filtered_grad, following, taps, window, input_grad):
    tokens, channels = filtered_grad.shape
    count = taps.shape[0]

    def each(index, carry):
        here = chunk_of(index)
        window[0:tokens, :] = filtered_grad[:, here]
        window[tokens : tokens + 8, :] = following[:, here]
        total = taps[count - 1 : count, here] * window[0:tokens, :]
        for k in range(count - 1):
            offset = count - 1 - k
            total = total + taps[k : k + 1, here] * window[offset : offset + tokens, :]
        input_grad[:, here] = total.astype(BF16)
        return carry

    lax.fori_loop(0, channels // LANES, each, 0)


def toggled(index, bit):
    return index + bit - 2 * bit * (index // bit % 2)


def weight_phase(columns, cotangents, total):
    peers, tokens, rows = columns.shape

    def each(index, carry):
        here = chunk_of(index)
        found = dot(columns[0, :, here], cotangents[0], TN)
        for peer in range(1, peers):
            found = found + dot(columns[peer, :, here], cotangents[peer], TN)
        total[pl.ds(pl.multiple_of(index * LANES, LANES), LANES), :] = found
        return carry

    lax.fori_loop(0, rows // LANES, each, 0)


def layer_kernel(
    spans, groups,
    raw, gate, step, taps, bias, step_bias, decay_log, decay_row, skip_wide, norm_weight,
    weight, cotangent,
    input_grad, gate_grad, step_grad, weight_grad, small,
    halo, weights, cotangents, act, slope, cum_wide, dt_wide, decay_wide, other_decay,
    cum_rows, cum_cols, dt_cols, key_t, query_t, window, scores,
    states, states_other, entering, inside, gated, scale, low, columns,
    normed_grad, scanned_grad, norm_grad, skip_sum,
    back_states, back_other, end_grad, score_grad, query_grad, row_sums, key_grad,
    filter_sums, head_sums, following, heads_out,
    weight_out, weight_in, weight_all, small_in,
    local_sem, halo_sem, decay_sem, gather_sem, column_sem, ahead_sem, back_sem, next_sem,
    share_sem, small_sem,
):
    q, d = lax.axis_index("seq"), lax.axis_index("dp")
    tokens, channels = raw.shape
    inner = gate.shape[1]
    own_rows = weight.shape[0]
    count = taps.shape[0]
    filtered_grad = act
    scaled_grad = normed_grad

    def remote(source, target, sems, slot, seq=None, dp=None):
        return pltpu.make_async_remote_copy(
            src_ref=source,
            dst_ref=target,
            send_sem=sems.at[0, slot],
            recv_sem=sems.at[1, slot],
            device_id=(q if seq is None else seq, d if dp is None else dp),
            device_id_type=MESH,
        )

    first, last = q == 0, q == spans - 1
    partner = toggled(q, 1)
    odd = q % 2 == 1
    group, groups_along = q // 2, spans // 2

    own_slot = pl.ds(pl.multiple_of(d * own_rows, LANES), own_rows)
    load_weight = pltpu.make_async_copy(weight, weights.at[own_slot], local_sem.at[0])
    load_cotangent = pltpu.make_async_copy(cotangent, cotangents.at[d], local_sem.at[1])
    load_weight.start()
    load_cotangent.start()

    halo_copy = remote(raw.at[tokens - 16 : tokens], halo, halo_sem, 0, seq=q + 1)
    pl.when(jnp.logical_not(last))(halo_copy.start)

    @pl.when(first)
    def _():
        halo[...] = jnp.zeros_like(halo)

    across, beside = toggled(d, 2), toggled(d, 1)

    def slot_of(owner):
        return weights.at[pl.ds(pl.multiple_of(owner * own_rows, LANES), own_rows)]

    def gather(kind, owner, slot, target):
        place = slot_of(owner) if kind == 0 else cotangents.at[owner]
        return remote(place, place, gather_sem, 3 * kind + slot, dp=target)

    load_weight.wait()
    load_cotangent.wait()
    for kind in range(2):
        gather(kind, d, 0, across).start()
        gather(kind, d, 1, beside).start()

    step_phase(step, step_bias, decay_log, cum_rows, cum_cols, dt_cols)
    expand_phase(cum_cols, dt_cols, cum_wide, dt_wide, decay_wide)
    decay_copy = remote(decay_wide, other_decay, decay_sem, 0, seq=partner)
    decay_copy.start()
    pl.when(jnp.logical_not(first))(halo_copy.wait_recv)

    def message(index):
        return pl.ds(index * GROUP, GROUP)

    def pair_copy(source, target, sems, index):
        return remote(source.at[message(index)], target.at[message(index)], sems, index, seq=partner)

    state_phase(
        raw, halo, taps, bias, window, act, slope, cum_wide, dt_wide, key_t, query_t, states,
        lambda index: pair_copy(states, states_other, ahead_sem, index).start(),
    )
    decay_copy.wait()
    score_blocks(act, inner, scores)

    def chain_step(index, own, other, arrived, pair_sem, chain_sem, late, begins, ends, towards):
        pair = pair_copy(own, other, pair_sem, index)
        chain = remote(own.at[message(index)], arrived.at[message(index)], chain_sem, index, seq=towards)
        pair.wait()
        pl.when(jnp.logical_not(begins))(chain.wait_recv)
        for j in range(GROUP):
            at = index * GROUP + j
            here = chunk_of(at)
            mine, theirs = own[at], other[at]
            mine_decay = decay_wide[0:1, here]
            their_decay = other_decay[0:1, here]
            running = jnp.where(begins, 0.0, arrived[at])
            both = jnp.where(late, mine_decay * theirs + mine, their_decay * mine + theirs)
            own[at] = mine_decay * their_decay * running + both
            arrived[at] = jnp.where(late, theirs + their_decay * running, running)
        pl.when(jnp.logical_not(ends))(chain.start)

    def chain_end(index, own, arrived, chain_sem, ends, towards):
        chain = remote(own.at[message(index)], arrived.at[message(index)], chain_sem, index, seq=towards)
        pl.when(jnp.logical_not(ends))(chain.wait_send)

    messages = states.shape[0] // GROUP
    begins, ends = group == 0, group == groups_along - 1

    inside_phase(
        act, cum_wide, dt_wide, cum_rows, scores, inside,
        lambda index: chain_step(
            index, states, states_other, entering, ahead_sem, next_sem.at[0], odd, begins, ends, q + 2
        ),
    )

    gather(0, across, 0, across).wait_recv()
    gather(0, across, 2, beside).start()
    norm_phase(act, cum_wide, inside, entering, skip_wide, gate, norm_weight, gated, scale, low)

    def column_copy(slot, peer):
        return remote(low.at[peer], columns.at[d], column_sem, slot, dp=peer)

    def column_arrival(slot, peer):
        return remote(low.at[peer], columns.at[peer], column_sem, slot, dp=peer)

    peers = (across, toggled(across, 1), beside)
    for slot, peer in enumerate(peers):
        column_copy(slot, peer).start()
    columns[d] = low[d]
    gather(1, across, 0, across).wait_recv()
    gather(1, across, 2, beside).start()
    gather(0, beside, 1, beside).wait_recv()
    gather(0, toggled(across, 1), 2, beside).wait_recv()

    gate_phase(
        act, cum_wide, inside, skip_wide, gate, norm_weight, gated, scale, query_t,
        cotangents.at[d], weights, normed_grad, scanned_grad, gate_grad, norm_grad, skip_sum,
        back_states,
        lambda index: pair_copy(back_states, back_other, back_sem, index).start(),
    )

    bits = []
    while 2 ** len(bits) < spans:
        bits.append(2 ** len(bits))
    size = own_rows
    base = 0
    plan = []
    offset = 0
    for bit in bits:
        mine = q // bit % 2
        if size // 2 % 16 == 0:
            size = size // 2
            keep, give = base + mine * size, base + (1 - mine) * size
            plan.append((bit, True, size, keep, give, offset, mine))
            base = keep
        else:
            plan.append((bit, False, size, base, base, offset, mine))
        offset = offset + size

    def rows_at(start, length):
        return pl.ds(pl.multiple_of(start, 16), length)

    def share_copy(number):
        bit, _, length, _, _, place, _ = plan[number]
        return remote(
            weight_out.at[place : place + length], weight_in.at[place : place + length],
            share_sem, number, seq=toggled(q, bit),
        )

    def share_start(number):
        _, _, length, _, give, place, _ = plan[number]
        weight_out[place : place + length] = weight_grad[rows_at(give, length)].astype(BF16)
        share_copy(number).start()

    def share_finish(number):
        _, halves, length, keep, _, place, _ = plan[number]
        share_copy(number).wait()
        found = weight_in[place : place + length].astype(F32)
        kept = weight_grad[rows_at(keep, length)]
        if not halves:
            kept = weight_out[place : place + length].astype(F32)
        weight_grad[rows_at(keep, length)] = kept + found

    def weights_ready():
        for slot, peer in enumerate(peers):
            column_arrival(slot, peer).wait_recv()
        gather(1, beside, 1, beside).wait_recv()
        gather(1, toggled(across, 1), 2, beside).wait_recv()
        weight_phase(columns, cotangents, weight_grad)
        share_start(0)

    def back_step(index):
        chain_step(
            index, back_states, back_other, end_grad, back_sem, next_sem.at[1],
            jnp.logical_not(odd), ends, begins, q - 2,
        )
        pl.when(index == messages // 2)(weights_ready)

    inside_grad_phase(
        act, cum_wide, dt_wide, cum_rows, scores, inside, scanned_grad, entering,
        scaled_grad, score_grad, query_grad, row_sums, back_step,
    )
    share_finish(0)
    if len(plan) > 1:
        share_start(1)
    end_phase(
        act, slope, cum_wide, dt_wide, cum_cols, dt_cols, decay_wide, skip_wide, scanned_grad,
        scaled_grad, score_grad, query_grad, row_sums, entering, end_grad, key_grad, skip_sum,
        step, step_bias, decay_row, raw, halo, taps, window, filtered_grad,
        step_grad, filter_sums, head_sums,
    )
    heads_out[...] = filtered_grad[0:8, :]
    back_copy = remote(heads_out, following, halo_sem, 1, seq=q - 1)
    pl.when(jnp.logical_not(first))(back_copy.start)

    @pl.when(last)
    def _():
        following[...] = jnp.zeros_like(following)

    small[...] = filter_sums[...]
    small[count + 1 : count + 2, 0:inner] = norm_grad[0:1, :]
    for row in range(3):
        small[count + 2 : count + 3, row * LANES : (row + 1) * LANES] = head_sums[row : row + 1, :]

    steps = [("dp", bit) for bit in (1, 2)] + [("seq", bit) for bit in bits]

    def small_copy(number):
        axis, bit = steps[number]
        target = {"seq": toggled(q, bit)} if axis == "seq" else {"dp": toggled(d, bit)}
        return remote(small_in.at[2 * number], small_in.at[2 * number + 1], small_sem, number, **target)

    def small_start(number):
        small_in[2 * number] = small[...]
        small_copy(number).start()

    def small_finish(number):
        small_copy(number).wait()
        small[...] += small_in[2 * number + 1]

    small_start(0)
    for number in range(1, len(plan)):
        share_finish(number)
        if number + 1 < len(plan):
            share_start(number + 1)
        small_finish(number - 1)
        small_start(number)

    final = plan[-1]
    weight_all[rows_at(base, size)] = weight_grad[rows_at(base, size)].astype(BF16)

    halvings = [number for number in range(len(plan)) if plan[number][1]]

    def spread_copy(number):
        bit, _, length, keep, _, _, _ = plan[number]
        place = weight_all.at[rows_at(keep, length)]
        return remote(place, place, share_sem, len(plan) + number, seq=toggled(q, bit))

    def spread_arrival(number):
        bit, _, length, _, give, _, _ = plan[number]
        place = weight_all.at[rows_at(give, length)]
        return remote(place, place, share_sem, len(plan) + number, seq=toggled(q, bit))

    spread_copy(halvings[-1]).start()
    pl.when(jnp.logical_not(last))(back_copy.wait_recv)
    filter_grad_phase(filtered_grad, following, taps, window, input_grad)
    for number in reversed(halvings):
        spread_arrival(number).wait_recv()
        if number > 0:
            spread_copy(number - 1).start()
    done = len(plan) - 1
    small_finish(done)
    for number in range(done + 1, len(steps)):
        small_start(number)
        small_finish(number)

    def widen(index, carry):
        rows = pl.ds(pl.multiple_of(index * 64, 64), 64)
        weight_grad[rows] = weight_all[rows].astype(F32)
        return carry

    lax.fori_loop(0, own_rows // 64, widen, 0)

    for number in halvings:
        spread_copy(number).wait_send()
    for kind in range(2):
        gather(kind, d, 0, across).wait_send()
        gather(kind, d, 1, beside).wait_send()
        gather(kind, across, 2, beside).wait_send()
    for slot, peer in enumerate(peers):
        column_copy(slot, peer).wait_send()
    pl.when(jnp.logical_not(last))(halo_copy.wait_send)
    pl.when(jnp.logical_not(first))(back_copy.wait_send)
    for index in range(messages):
        chain_end(index, states, entering, next_sem.at[0], ends, q + 2)
        chain_end(index, back_states, end_grad, next_sem.at[1], begins, q - 2)


def body(
    conv_input,
    gate_input,
    step_input,
    filter_taps,
    filter_bias,
    step_bias,
    decay_log,
    skip_gain,
    norm_weight,
    output_weight,
    output_grad,
):
    raw, gate, step, cotangent = conv_input[0], gate_input[0], step_input[0], output_grad[0]
    tokens, channels = raw.shape
    inner = gate.shape[1]
    heads = step.shape[0]
    own_rows, width = output_weight.shape
    count = filter_taps.shape[0]
    spans, groups = lax.axis_size("seq"), lax.axis_size("dp")
    half = tokens // 2
    chunks = inner // LANES
    messages = chunks // GROUP
    assert groups == 4 and tokens % 256 == 0 and inner % (GROUP * LANES) == 0
    levels = spans.bit_length() - 1
    shared, size = 0, own_rows
    for _ in range(levels):
        size = size // 2 if size // 2 % 16 == 0 else size
        shared += size
    wide = pltpu.VMEM((tokens, inner), F32)
    full = pltpu.VMEM((tokens, channels), F32)
    columns = pltpu.VMEM((tokens, LANES), F32)
    row8 = pltpu.VMEM((8, inner), F32)
    stored = pltpu.VMEM((chunks, LANES, LANES), F32)
    turned = pltpu.VMEM((2, LANES, tokens), BF16)
    squares = pltpu.VMEM((3, half, half), F32)
    edge = pltpu.VMEM((8, channels), F32)
    sems = pltpu.SemaphoreType.DMA
    scratch = [
        pltpu.VMEM((16, channels), BF16),
        pltpu.VMEM((groups * own_rows, width), BF16),
        pltpu.VMEM((groups, tokens, width), BF16),
        full, full, wide, wide, row8, row8,
        pltpu.VMEM((heads, 1, tokens), F32), columns, columns, turned, turned,
        pltpu.VMEM((tokens + 8, LANES), F32), squares,
        stored, stored, stored, wide, wide, columns,
        pltpu.VMEM((groups, tokens, own_rows), BF16),
        pltpu.VMEM((groups, tokens, own_rows), BF16),
        wide, wide, row8, row8,
        stored, stored, stored, squares, columns, columns, columns,
        edge, pltpu.VMEM((8, LANES), F32), edge, edge,
        pltpu.VMEM((shared, width), BF16),
        pltpu.VMEM((shared, width), BF16),
        pltpu.VMEM((own_rows, width), BF16),
        pltpu.VMEM((2 * (levels + 2), 8, channels), F32),
        sems((2,)), sems((2, 2)), sems((2, 1)), sems((2, 6)), sems((2, 3)),
        sems((2, messages)), sems((2, messages)), sems((2, 2, messages)),
        sems((2, 2 * levels)), sems((2, levels + 2)),
    ]
    outs = [
        ((tokens, channels), BF16), ((tokens, inner), BF16), ((heads, tokens), F32),
        ((own_rows, width), F32), ((8, channels), F32),
    ]
    args = (
        raw, gate, step, filter_taps, filter_bias[None], step_bias[:, None], decay_log[:, None],
        jnp.pad(decay_log, (0, LANES - heads))[None], jnp.repeat(skip_gain, HEAD_DIM)[None],
        norm_weight[None], output_weight, cotangent,
    )
    vmem = pl.BlockSpec(memory_space=pltpu.VMEM)
    anywhere = pl.BlockSpec(memory_space=pl.ANY)
    input_grad, gate_grad, step_grad, weight_grad, small = pl.pallas_call(
        functools.partial(layer_kernel, spans, groups),
        out_shape=[jax.ShapeDtypeStruct(shape, kind) for shape, kind in outs],
        in_specs=[vmem] * (len(args) - 2) + [anywhere] * 2,
        out_specs=[vmem] * len(outs),
        scratch_shapes=scratch,
        compiler_params=pltpu.CompilerParams(
            vmem_limit_bytes=67043328, has_side_effects=True
        ),
    )(*args)
    head_grads = small[count + 2, : 3 * LANES].reshape(3, LANES)[:, :heads]
    return (
        input_grad[None], gate_grad[None], step_grad[None], weight_grad,
        small[: count + 1], small[count + 1, :inner], head_grads,
    )


def solution(mesh):
    return jax.shard_map(
        body,
        mesh=mesh,
        in_specs=(
            P("dp", "seq", None),
            P("dp", "seq", None),
            P("dp", None, "seq"),
            P(),
            P(),
            P(),
            P(),
            P(),
            P(),
            P("dp", None),
            P("dp", "seq", None),
        ),
        out_specs=(
            P("dp", "seq", None),
            P("dp", "seq", None),
            P("dp", None, "seq"),
            P("dp", None),
            P(),
            P(),
            P(),
        ),
        check_vma=False,
    )
```

```python
import functools

import jax
import jax.numpy as jnp
from jax import lax
from jax.experimental import pallas as pl
from jax.experimental.pallas import tpu as pltpu
from jax.sharding import PartitionSpec as P

F32 = jnp.float32
BF16 = jnp.bfloat16
EPSILON = 1e-05
LOG2E = 1.4426950408889634
LANES = 128
HEAD_DIM = 64
MESH = pl.DeviceIdType.MESH
CHAIN_HOOKS = (6, 9)
FAR_HOOKS = (4, 8)
NEAR_HOOKS = (6, 9)
NN = (((1,), (0,)), ((), ()))
NT = (((1,), (1,)), ((), ()))
TN = (((0,), (0,)), ((), ()))


def dot(a, b, dims=NN):
    return lax.dot_general(a, b, dims, preferred_element_type=F32)


def rounded_high(a):
    scaled = a * 65537.0
    return scaled - (scaled - a)


def split2(a):
    high = rounded_high(a)
    return high.astype(BF16), (a - high).astype(BF16)


def split3(a):
    high = rounded_high(a)
    rest = a - high
    middle = rounded_high(rest)
    return high.astype(BF16), middle.astype(BF16), (rest - middle).astype(BF16)


def dot3(a, b, dims=NN):
    return dot(a[0], b[0], dims) + (dot(a[0], b[1], dims) + dot(a[1], b[0], dims))


def chunk_of(index):
    return pl.ds(pl.multiple_of(index * LANES, LANES), LANES)


def iota(shape, dim):
    return lax.broadcasted_iota(jnp.int32, shape, dim)


def low_half(shape):
    return iota(shape, 1) < HEAD_DIM


def head_rows(index):
    shape = (LANES, LANES)
    wanted = 2 * index + jnp.where(low_half(shape), 0, 1)
    return jnp.where(iota(shape, 0) == wanted, 1.0, 0.0).astype(BF16)


def sigmoid(a):
    return 1.0 / (1.0 + jnp.exp(-a))


def transposed(rows):
    heads, tokens = rows.shape
    padded = jnp.concatenate([rows, jnp.zeros((LANES - heads, tokens), F32)], axis=0)
    return padded.T


def padded_row(row):
    short = row[...]
    return jnp.concatenate([short, jnp.zeros((1, LANES - short.shape[1]), F32)], axis=1)


def column_of(row):
    return jnp.broadcast_to(padded_row(row), (LANES, LANES)).T[: row.shape[1], 0:1]


def step_phase(step, step_bias, decay_log, cum_rows, cum_cols, dt_cols):
    shifted = step[...] + column_of(step_bias)
    sizes = jnp.maximum(shifted, 0.0) + jnp.log1p(jnp.exp(-jnp.abs(shifted)))
    rates = -jnp.exp(column_of(decay_log)) * sizes
    tokens = rates.shape[1]
    shape = (tokens, tokens)
    before = jnp.where(iota(shape, 0) <= iota(shape, 1), 1.0, 0.0).astype(BF16)
    high, middle, low = split3(rates)
    cumulative = (dot(high, before) + (dot(middle, before) + dot(low, before))) * LOG2E
    for head in range(rates.shape[0]):
        cum_rows[head] = cumulative[head : head + 1]
    cum_cols[...] = transposed(cumulative)
    dt_cols[...] = transposed(sizes)


def expand_phase(cum_cols, dt_cols, skip_gain, cum_wide, dt_wide, decay_wide, skip_wide):
    tokens, inner = cum_wide.shape
    cum_parts = split3(cum_cols[...])
    dt_parts = split3(dt_cols[...])
    skip_parts = split3(jnp.broadcast_to(padded_row(skip_gain), (8, LANES)))

    def each(index, carry):
        here = chunk_of(index)
        rows = head_rows(index)
        wide = dot(cum_parts[0], rows) + (dot(cum_parts[1], rows) + dot(cum_parts[2], rows))
        cum_wide[:, here] = wide
        skip_wide[:, here] = dot(skip_parts[0], rows) + (
            dot(skip_parts[1], rows) + dot(skip_parts[2], rows)
        )
        dt_wide[:, here] = dot(dt_parts[0], rows) + (
            dot(dt_parts[1], rows) + dot(dt_parts[2], rows)
        )
        decay_wide[:, here] = jnp.broadcast_to(jnp.exp2(wide[tokens - 1 : tokens]), (8, LANES))
        return carry

    lax.fori_loop(0, inner // LANES, each, 0, unroll=4)


def filter_chunk(index, slot, here, raw, halo, taps, bias, windows, act, slope):
    tokens = raw.shape[0]
    window = windows.at[slot]
    window[0:8, :] = halo[:, here].astype(F32)[8:]
    window[8 : 8 + tokens, :] = raw[:, here].astype(F32)
    count = taps.shape[0]
    filtered = bias[pl.ds(index, 1), :] + taps[0:1, here] * window[9 - count : 9 - count + tokens, :]
    for k in range(1, count):
        filtered = filtered + taps[k : k + 1, here] * window[9 - count + k : 9 - count + k + tokens, :]
    gate = sigmoid(filtered)
    result = filtered * gate
    act[:, here] = result
    slope[:, here] = gate + result * (1.0 - gate)
    return result


def in_pairs(total, before, after, each, carry):
    def several(number, carry):
        if before is not None:
            before(number)
        for j in range(2):
            carry = each(2 * number + j, carry, j)
        if after is not None:
            after(number)
        return carry

    return lax.fori_loop(0, total // 2, several, carry)


def state_phase(
    raw, halo, taps, bias, window, act, slope, cum_wide, dt_wide, key_t, query_t, states, after
):
    tokens, inner = cum_wide.shape
    first = inner // LANES
    key = filter_chunk(first, 0, pl.ds(inner, LANES), raw, halo, taps, bias, window, act, slope)
    query = filter_chunk(first + 1, 1, pl.ds(inner + LANES, LANES), raw, halo, taps, bias, window, act, slope)
    high, low = split2(key.T)
    key_t[0], key_t[1] = high, low
    high, low = split2(query.T)
    query_t[0], query_t[1] = high, low

    def each(index, carry, slot):
        here = chunk_of(index)
        values = filter_chunk(index, slot, here, raw, halo, taps, bias, window, act, slope)
        cum = cum_wide[:, here]
        moved = values * dt_wide[:, here] * jnp.exp2(cum[tokens - 1 : tokens] - cum)
        states[index] = dot3((key_t[0], key_t[1]), split2(moved))
        return carry

    in_pairs(first, None, after, each, 0)


def score_blocks(act, inner, scores):
    half = act.shape[0] // 2
    key = split2(act[:, inner : inner + LANES])
    query = split2(act[:, inner + LANES : inner + 2 * LANES])
    shape = (half, half)
    causal = iota(shape, 0) >= iota(shape, 1)
    for slot, (rows, columns) in enumerate(((0, 0), (1, 1), (1, 0))):
        left = tuple(part[rows * half : (rows + 1) * half] for part in query)
        right = tuple(part[columns * half : (columns + 1) * half] for part in key)
        block = dot3(left, right, NT)
        if rows == columns:
            block = jnp.where(causal, block, 0.0)
        scores[slot] = block


def decay_blocks(index, cum, cum_rows, half, block):
    rows = slice(block * half, (block + 1) * half)
    found = []
    for j in range(2):
        column = jnp.broadcast_to(cum[rows, j * HEAD_DIM : j * HEAD_DIM + 1], (half, half))
        row = cum_rows[2 * index + j][:, rows]
        found.append(jnp.exp2(jnp.minimum(column - row, 0.0)))
    return jnp.concatenate(found, axis=1)


def stacked(block):
    low = low_half(block.shape)
    zero = jnp.zeros_like(block)
    return jnp.concatenate([jnp.where(low, block, zero), jnp.where(low, zero, block)], axis=0)


def inside_phase(act, cum_wide, dt_wide, cum_rows, scores, inside, before, after):
    tokens, inner = cum_wide.shape
    half = tokens // 2

    def each(index, carry, slot):
        here = chunk_of(index)
        scaled = act[:, here] * dt_wide[:, here]
        cum = cum_wide[:, here]
        for block in range(2):
            rows = slice(block * half, (block + 1) * half)
            weights = decay_blocks(index, cum, cum_rows, half, block)
            score = scores[block]
            weights = jnp.concatenate([score, score], axis=1) * weights
            right = stacked(scaled[rows])
            result = dot3(split2(weights), split2(right))
            if block == 1:
                middle = cum[half - 1 : half]
                moved = scaled[:half] * jnp.exp2(middle - cum[:half])
                result = result + jnp.exp2(cum[half:] - middle) * dot3(
                    split2(scores[2]), split2(moved)
                )
            inside[rows, here] = result
        return carry

    in_pairs(inner // LANES, before, after, each, 0)


def norm_phase(act, cum_wide, inside, entering, skip_wide, gate, norm_weight, gated, scale, low):
    tokens, inner = cum_wide.shape
    query = split2(act[:, inner + LANES : inner + 2 * LANES])

    def each(index, total):
        here = chunk_of(index)
        crossed = jnp.exp2(cum_wide[:, here]) * dot3(query, split2(entering[index]))
        scanned = inside[:, here] + crossed
        inside[:, here] = scanned
        scanned = scanned + skip_wide[0:1, here] * act[:, here]
        branch = gate[:, here].astype(F32)
        result = scanned * (branch * sigmoid(branch))
        gated[:, here] = result
        return total + result * result

    total = lax.fori_loop(0, inner // LANES, each, jnp.zeros((tokens, LANES), F32), unroll=2)
    mean = jnp.sum(total, axis=1, keepdims=True) / inner
    inverse = lax.rsqrt(mean + EPSILON)
    scale[...] = jnp.broadcast_to(inverse, scale.shape)

    per = low.shape[2] // LANES

    def rounded(index, carry):
        here = chunk_of(index)
        place = pl.ds(pl.multiple_of(index % per * LANES, LANES), LANES)
        result = gated[:, here] * scale[...] * norm_weight[pl.ds(index, 1), :]
        low[index // per, :, place] = result.astype(BF16)
        return carry

    lax.fori_loop(0, inner // LANES, rounded, 0)


def gate_phase(
    act, cum_wide, inside, skip_wide, gate, norm_weight, gated, scale, query_t,
    chip, normed_sent, normed_grad, scanned_grad, gate_grad, norm_grad, skip_sum, entering_grad,
    after,
):
    tokens, inner = cum_wide.shape

    per = normed_grad.shape[2] // LANES

    def normed_at(index):
        return normed_grad[index // per, :, chunk_of(index % per)]

    def first(index, total):
        here = chunk_of(index)
        slot, place = index // per, chunk_of(index % per)
        sent = normed_sent[slot, :, place].astype(F32)
        found = jnp.where(slot // 2 == chip, normed_grad[slot, :, place], sent)
        normed_grad[slot, :, place] = found
        return total + found * norm_weight[pl.ds(index, 1), :] * gated[:, here]

    total = lax.fori_loop(0, inner // LANES, first, jnp.zeros((tokens, LANES), F32), unroll=2)
    inverse = scale[...]
    pull = jnp.sum(total, axis=1, keepdims=True) / inner * inverse * inverse * inverse

    def second(index, carry, slot):
        here = chunk_of(index)
        found = normed_at(index)
        product = gated[:, here]
        norm_grad[:, here] = jnp.broadcast_to(
            jnp.sum(found * product * inverse, axis=0, keepdims=True), (8, LANES)
        )
        down = inverse * (found * norm_weight[pl.ds(index, 1), :]) - product * pull
        branch = gate[:, here].astype(F32)
        opened = sigmoid(branch)
        passed = branch * opened
        values = act[:, here]
        scanned = inside[:, here] + skip_wide[0:1, here] * values
        gate_grad[:, here] = (down * scanned * (opened + passed * (1.0 - opened))).astype(BF16)
        back = down * passed
        scanned_grad[:, here] = back
        skip_sum[:, here] = jnp.broadcast_to(
            jnp.sum(back * values, axis=0, keepdims=True), (8, LANES)
        )
        moved = back * jnp.exp2(cum_wide[:, here])
        entering_grad[index] = dot3((query_t[0], query_t[1]), split2(moved))
        return carry

    in_pairs(inner // LANES, None, after, second, 0)


def inside_grad_phase(
    act, cum_wide, dt_wide, cum_rows, scores, inside, scanned_grad, entering,
    scaled_grad, score_grad, query_grad, row_sums, before, after,
):
    tokens, inner = cum_wide.shape
    half = tokens // 2
    score_grad[...] = jnp.zeros_like(score_grad)
    query_grad[...] = jnp.zeros_like(query_grad)
    row_sums[...] = jnp.zeros_like(row_sums)

    def each(index, carry, slot):
        here = chunk_of(index)
        scaled = act[:, here] * dt_wide[:, here]
        cum = cum_wide[:, here]
        back = scanned_grad[:, here]
        middle = cum[half - 1 : half]
        for block in range(2):
            rows = slice(block * half, (block + 1) * half)
            decay = decay_blocks(index, cum, cum_rows, half, block)
            score = scores[block]
            weights = split2(jnp.concatenate([score, score], axis=1) * decay)
            down = split2(back[rows])
            products = dot3(down, split2(stacked(scaled[rows])), NT) * decay
            score_grad[block] += products[:, :half] + products[:, half:]
            found = dot3(weights, down, TN)
            found = jnp.where(low_half((half, LANES)), found[:half], found[half:])
            if block == 0:
                pulled = split2(back[half:] * jnp.exp2(cum[half:] - middle))
                factor = jnp.exp2(middle - cum[:half])
                score_grad[2] += dot3(pulled, split2(scaled[:half] * factor), NT)
                found = found + factor * dot3(split2(scores[2]), pulled, TN)
            scaled_grad[rows, here] = found
        query_grad[...] += dot3(split2(back * jnp.exp2(cum)), split2(entering[index]), NT)
        rows = head_rows(index)
        high, low = split2(back * inside[:, here])
        row_sums[...] += dot(high, rows, NT) + dot(low, rows, NT)
        return carry

    in_pairs(inner // LANES, before, after, each, 0)


def end_phase(
    act, slope, cum_wide, dt_wide, cum_cols, dt_cols, decay_wide, skip_wide, scanned_grad,
    scaled_grad, score_grad, query_grad, row_sums, entering, end_grad, key_grad, skip_sum,
    step, step_bias, decay_log, raw, halo, taps, windows, filtered_grad,
    step_grad, filter_sums, head_sums, before_pair, after_pair,
):
    tokens, inner = cum_wide.shape
    half = tokens // 2
    key = split2(act[:, inner : inner + LANES])
    query = split2(act[:, inner + LANES : inner + 2 * LANES])
    count = taps.shape[0]

    def finish(slot, here, found):
        pulled = found * slope[:, here]
        filtered_grad[:, here] = pulled
        window = windows.at[slot]
        window[0:8, :] = halo[:, here].astype(F32)[8:]
        window[8 : 8 + tokens, :] = raw[:, here].astype(F32)
        sums = [
            jnp.sum(pulled * window[9 - count + k : 9 - count + k + tokens, :], axis=0, keepdims=True)
            for k in range(count)
        ]
        sums.append(jnp.sum(pulled, axis=0, keepdims=True))
        sums.append(jnp.zeros((8 - len(sums), LANES), F32))
        filter_sums[:, here] = jnp.concatenate(sums, axis=0)

    key_grad[...] = jnp.zeros_like(key_grad)
    zeros = (jnp.zeros((tokens, LANES), F32), jnp.zeros((8, LANES), F32), jnp.zeros((8, LANES), F32))

    def each(index, sums, slot):
        value_sums, last_sums, skip_sums = sums
        here = chunk_of(index)
        values = act[:, here]
        sizes = dt_wide[:, here]
        cum = cum_wide[:, here]
        to_end = jnp.exp2(cum[tokens - 1 : tokens] - cum)
        after = end_grad[index]
        parts = split2(after)
        moved = values * sizes * to_end
        moved_grad = dot3(key, parts)
        key_grad[...] += dot3(split2(moved), parts, NT)
        last = jnp.sum(moved * moved_grad, axis=0, keepdims=True) + decay_wide[0:1, here] * jnp.sum(
            after * entering[index], axis=0, keepdims=True
        )
        scaled = scaled_grad[:, here] + to_end * moved_grad
        rows = head_rows(index)
        high, low = split2(scaled * values)
        value_sums = value_sums + (dot(high, rows, NT) + dot(low, rows, NT))
        parts = split3(jnp.broadcast_to(last, (8, LANES)))
        last_sums = last_sums + (dot(parts[0], rows, NT) + (dot(parts[1], rows, NT) + dot(parts[2], rows, NT)))
        parts = split3(skip_sum[:, here])
        skip_sums = skip_sums + (dot(parts[0], rows, NT) + (dot(parts[1], rows, NT) + dot(parts[2], rows, NT)))
        finish(slot, here, scaled * sizes + skip_wide[0:1, here] * scanned_grad[:, here])
        return value_sums, last_sums, skip_sums

    value_sums, last_sums, skip_sums = in_pairs(inner // LANES, before_pair, after_pair, each, zeros)

    shape = (half, half)
    causal = iota(shape, 0) >= iota(shape, 1)
    blocks = [split2(jnp.where(causal, score_grad[slot], 0.0)) for slot in range(2)]
    blocks.append(split2(score_grad[2]))
    first = lambda parts: tuple(part[:half] for part in parts)
    second = lambda parts: tuple(part[half:] for part in parts)
    upper = dot3(blocks[0], first(key))
    lower = dot3(blocks[1], second(key)) + dot3(blocks[2], first(key))
    finish(1, pl.ds(inner + LANES, LANES), query_grad[...] + jnp.concatenate([upper, lower], axis=0))
    upper = dot3(blocks[0], first(query), TN) + dot3(blocks[2], second(query), TN)
    lower = dot3(blocks[1], second(query), TN)
    finish(0, pl.ds(inner, LANES), key_grad[...] + jnp.concatenate([upper, lower], axis=0))

    sizes = dt_cols[...]
    cum_grad = row_sums[...] - sizes * value_sums
    at_end = iota((tokens, LANES), 0) == tokens - 1
    cum_grad = cum_grad + jnp.where(at_end, jnp.broadcast_to(last_sums[0:1], (tokens, LANES)), 0.0)
    shape = (tokens, tokens)
    after = jnp.where(iota(shape, 0) <= iota(shape, 1), 1.0, 0.0).astype(BF16)
    parts = split3(cum_grad)
    rate_grad = dot(after, parts[0]) + (dot(after, parts[1]) + dot(after, parts[2]))
    rate = -jnp.exp(padded_row(decay_log))
    heads = step.shape[0]
    shifted = transposed(step[...] + column_of(step_bias))
    pulled = (value_sums + rate_grad * rate) * sigmoid(shifted)
    pulled = jnp.where(iota((tokens, LANES), 1) < heads, pulled, 0.0)
    step_grad[...] = pulled.T[:heads]
    head_sums[...] = jnp.concatenate(
        [
            jnp.sum(pulled, axis=0, keepdims=True),
            jnp.sum(rate_grad * rate * sizes, axis=0, keepdims=True),
            skip_sums[0:1],
            jnp.zeros((5, LANES), F32),
        ],
        axis=0,
    )


def filter_grad_phase(filtered_grad, following, taps, windows, input_grad):
    tokens, channels = filtered_grad.shape
    count = taps.shape[0]

    def each(index, carry, slot):
        here = chunk_of(index)
        window = windows.at[slot]
        window[0:tokens, :] = filtered_grad[:, here]
        window[tokens : tokens + 8, :] = following[:, here]
        total = taps[count - 1 : count, here] * window[0:tokens, :]
        for k in range(count - 1):
            offset = count - 1 - k
            total = total + taps[k : k + 1, here] * window[offset : offset + tokens, :]
        input_grad[:, here] = total.astype(BF16)
        return carry

    in_pairs(channels // LANES, None, None, each, 0)


def toggled(index, bit):
    return index + bit - 2 * bit * (index // bit % 2)


def weight_phase(columns, cotangents, total):
    peers, tokens, rows = columns.shape

    def each(index, carry):
        here = chunk_of(index)
        found = dot(columns[0, :, here], cotangents[0], TN)
        for peer in range(1, peers):
            found = found + dot(columns[peer, :, here], cotangents[peer], TN)
        total[pl.ds(pl.multiple_of(index * LANES, LANES), LANES), :] = found
        return carry

    lax.fori_loop(0, rows // LANES, each, 0)


def layer_kernel(
    spans, groups,
    raw, step, taps, bias, step_bias, decay_log, skip_gain, norm_weight,
    weight, cotangent, gate_in,
    input_grad, gate_out, step_grad, weight_result, filter_out, norm_out, head_out,
    gate, gate_grad, weight_grad, small, skip_wide, halo, weights, cotangents, act, slope, cum_wide, dt_wide, decay_wide, other_decay,
    cum_rows, cum_cols, dt_cols, key_t, query_t, window, scores,
    states, states_other, entering, inside, gated, scale, low, columns,
    normed_grad, normed_sent, partial_beside, partials, scaled_grad, scanned_grad, norm_grad, skip_sum,
    back_states, back_other, end_grad, score_grad, query_grad, row_sums, key_grad,
    filter_sums, head_sums, following, heads_out,
    weight_out, weight_in, weight_all, small_in,
    local_sem, halo_sem, decay_sem, gather_sem, partial_sem, column_sem, ahead_sem, back_sem, next_sem, return_sem,
    share_sem, small_sem,
):
    q, d = lax.axis_index("seq"), lax.axis_index("dp")
    tokens, channels = raw.shape
    inner = gate_in.shape[1]
    own_rows = weight.shape[0]
    count = taps.shape[0]
    filtered_grad = act

    def remote(source, target, sems, slot, seq=None, dp=None):
        return pltpu.make_async_remote_copy(
            src_ref=source,
            dst_ref=target,
            send_sem=sems.at[0, slot],
            recv_sem=sems.at[1, slot],
            device_id=(q if seq is None else seq, d if dp is None else dp),
            device_id_type=MESH,
        )

    first, last = q == 0, q == spans - 1
    partner = toggled(q, 1)
    odd = q % 2 == 1
    group, groups_along = q // 2, spans // 2

    load_weight = pltpu.make_async_copy(weight, weights, local_sem.at[0])
    load_cotangent = pltpu.make_async_copy(cotangent, cotangents.at[d], local_sem.at[1])
    load_gate = pltpu.make_async_copy(gate_in, gate, local_sem.at[2])
    load_cotangent.start()
    load_weight.start()
    load_gate.start()

    across, beside = toggled(d, 2), toggled(d, 1)
    bits = []
    while 2 ** len(bits) < spans:
        bits.append(2 ** len(bits))
    barrier = pltpu.get_barrier_semaphore()

    def greet(seq, dp):
        pl.semaphore_signal(barrier, inc=1, device_id=(seq, dp), device_id_type=MESH)

    for other in (across, beside, toggled(across, 1)):
        greet(q, other)
    for bit in bits:
        greet(toggled(q, bit), d)
    expected = 3 + len(bits)
    for distance in (1, 2):
        below, above = q >= distance, q < spans - distance
        pl.when(below)(lambda distance=distance: greet(q - distance, d))
        pl.when(above)(lambda distance=distance: greet(q + distance, d))
        expected = expected + jnp.where(below, 1, 0) + jnp.where(above, 1, 0)

    with jax.named_scope("steps"):
        step_phase(step, step_bias, decay_log, cum_rows, cum_cols, dt_cols)
    with jax.named_scope("barrier"):
        pl.semaphore_wait(barrier, expected)

    with jax.named_scope("halo_start"):
        halo_copy = remote(raw.at[tokens - 16 : tokens], halo, halo_sem, 0, seq=q + 1)
    pl.when(jnp.logical_not(last))(halo_copy.start)

    @pl.when(first)
    def _():
        halo[...] = jnp.zeros_like(halo)

    diagonal = toggled(across, 1)

    def gather(owner, slot, target):
        place = cotangents.at[owner]
        return remote(place, place, gather_sem, slot, dp=target)

    load_cotangent.wait()
    gather(d, 0, across).start()
    gather(d, 1, beside).start()

    with jax.named_scope("expand"):
        expand_phase(cum_cols, dt_cols, skip_gain, cum_wide, dt_wide, decay_wide, skip_wide)
    decay_copy = remote(decay_wide, other_decay, decay_sem, 0, seq=partner)
    decay_copy.start()
    pl.when(jnp.logical_not(first))(halo_copy.wait_recv)

    side = q % 2

    def pair_copy(source, target, sems, number, arrival=False):
        at = 2 * number + (side if arrival else 1 - side)
        return remote(source.at[at], target.at[at], sems, number, seq=partner)

    with jax.named_scope("states"):
        state_phase(
            raw, halo, taps, bias, window, act, slope, cum_wide, dt_wide, key_t, query_t, states,
            lambda number: pair_copy(states, states_other, ahead_sem, number).start(),
        )
    with jax.named_scope("decay"):
        decay_copy.wait()
    score_blocks(act, inner, scores)

    def chain_copy(own, arrived, sems, number, towards):
        at = 2 * number + side
        return remote(own.at[at], arrived.at[at], sems, number, seq=towards)

    def return_copy(other, arrived, sems, number, arrival=False):
        at = 2 * number + (1 - side if arrival else side)
        return remote(other.at[at], arrived.at[at], sems, number, seq=partner)

    def chain_step(number, own, other, arrived, sems, late, begins, ends, towards):
        pair_sem, chain_sem, return_sem = sems
        chain = chain_copy(own, arrived, chain_sem, number, towards)
        with jax.named_scope("pair_wait"):
            pair_copy(own, other, pair_sem, number, arrival=True).wait_recv()
        with jax.named_scope("chain_wait"):
            pl.when(jnp.logical_not(begins))(chain.wait_recv)
        at = 2 * number + side
        here = chunk_of(at)
        mine, theirs = own[at], other[at]
        mine_decay, their_decay = decay_wide[0:1, here], other_decay[0:1, here]
        running = jnp.where(begins, 0.0, arrived[at])
        both = jnp.where(late, mine_decay * theirs + mine, their_decay * mine + theirs)
        own[at] = mine_decay * their_decay * running + both
        pl.when(jnp.logical_not(ends))(chain.start)
        arrived[at] = jnp.where(late, theirs + their_decay * running, running)
        other[at] = jnp.where(late, running, mine + mine_decay * running)
        return_copy(other, arrived, return_sem, number).start()

    def chain_end(number, own, other, arrived, sems, ends, towards):
        pair_sem, chain_sem, return_sem = sems
        pair_copy(own, other, pair_sem, number).wait_send()
        chain = chain_copy(own, arrived, chain_sem, number, towards)
        pl.when(jnp.logical_not(ends))(chain.wait_send)
        return_copy(other, arrived, return_sem, number).wait_send()

    messages = states.shape[0] // 2
    ahead_sems = (ahead_sem, next_sem.at[0], return_sem.at[0])
    back_sems = (back_sem, next_sem.at[1], return_sem.at[1])
    begins, ends = group == 0, group == groups_along - 1

    per_slot = own_rows // LANES
    owners = (d, beside, across, diagonal)
    load_weight.wait()

    def partial_copy(slot, arrival=False):
        owner = owners[slot]
        lands = owner if arrival else d
        if slot == 1:
            return remote(partial_beside, normed_grad.at[lands], partial_sem, 0, dp=owner)
        return remote(partials.at[slot - 2], normed_sent.at[lands], partial_sem, slot - 1, dp=owner)

    def partial_chunk(number):
        slot = number // per_slot
        owner = owners[3]
        for other in (2, 1, 0):
            owner = jnp.where(slot == other, owners[other], owner)
        index = number % per_slot
        rows = weights[pl.ds(pl.multiple_of(index * LANES, LANES), LANES), :]
        found = dot(cotangents[owner], rows, NT)

        @pl.when(slot == 0)
        def _():
            normed_grad[d, :, chunk_of(index)] = found

        @pl.when(slot == 1)
        def _():
            partial_beside[:, chunk_of(index)] = found

        @pl.when(slot > 1)
        def _():
            partials[slot - 2, :, chunk_of(index)] = found.astype(BF16)

        for slot in (1, 2, 3):
            pl.when(number == (slot + 1) * per_slot - 1)(partial_copy(slot).start)

    early = group < 2

    def across_arrives():
        gather(across, 0, across).wait_recv()
        gather(across, 2, beside).start()

    def ahead_before(number):
        @pl.when((number == 0) & jnp.logical_not(early))
        def _():
            gather(beside, 1, beside).wait_recv()

            def several(first, last):
                def each(at, carry):
                    partial_chunk(at)
                    return carry

                lax.fori_loop(first * per_slot, last * per_slot, each, 0)

            several(0, 2)
            across_arrives()
            several(2, 3)
            gather(diagonal, 2, beside).wait_recv()
            several(3, 4)

    def ahead_step(number):
        chain_step(
            number, states, states_other, entering, ahead_sems, odd, begins, ends, q + 2
        )

        @pl.when(early)
        def _():
            pl.when(number == per_slot // 2)(gather(beside, 1, beside).wait_recv)
            pl.when(number == per_slot)(across_arrives)
            pl.when(number == per_slot + per_slot // 2)(gather(diagonal, 2, beside).wait_recv)
            for j in range(2):
                partial_chunk(2 * number + j)

    with jax.named_scope("inside"):
        inside_phase(
            act, cum_wide, dt_wide, cum_rows, scores, inside, ahead_before, ahead_step,
        )

    with jax.named_scope("return_wait"):
        for number in range(messages):
            return_copy(states_other, entering, ahead_sems[2], number, arrival=True).wait_recv()
    load_gate.wait()
    with jax.named_scope("norm"):
        norm_phase(act, cum_wide, inside, entering, skip_wide, gate, norm_weight, gated, scale, low)

    def column_copy(slot, peer):
        return remote(low.at[peer], columns.at[d], column_sem, slot, dp=peer)

    def column_arrival(slot, peer):
        return remote(low.at[peer], columns.at[peer], column_sem, slot, dp=peer)

    peers = (across, diagonal, beside)
    for slot, peer in enumerate(peers):
        column_copy(slot, peer).start()
    columns[d] = low[d]
    with jax.named_scope("partial_wait"):
        for slot in (1, 2, 3):
            partial_copy(slot, arrival=True).wait_recv()

    with jax.named_scope("gate"):
        gate_phase(
            act, cum_wide, inside, skip_wide, gate, norm_weight, gated, scale, query_t,
            d // 2, normed_sent, normed_grad, scanned_grad, gate_grad, norm_grad, skip_sum,
            back_states,
            lambda number: pair_copy(back_states, back_other, back_sem, number).start(),
        )

    store_gate = pltpu.make_async_copy(gate_grad, gate_out, local_sem.at[0])
    store_gate.start()

    def plan_for(order):
        size, base, offset = own_rows, 0, 0
        plan = []
        for bit in order:
            mine = q // bit % 2
            halves = size // 2 % 16 == 0
            if halves:
                size = size // 2
                keep, give = base + mine * size, base + (1 - mine) * size
                base = keep
            else:
                keep, give = base, base
            plan.append((bit, halves, size, keep, give, offset))
            offset = offset + size
        return plan

    plans = (plan_for(bits), plan_for(bits[1:] + bits[:1]))
    levels = len(bits)
    halvings = [number for number in range(levels) if plans[0][number][1]]
    half_width = cotangent.shape[1] // 2

    def rows_at(start, length):
        return pl.ds(pl.multiple_of(start, 16), length)

    def lanes_of(part):
        return pl.ds(part * half_width, half_width)

    def share_copy(number, part):
        bit, _, length, _, _, place = plans[part][number]
        rows = pl.ds(place, length)
        return remote(
            weight_out.at[part, rows], weight_in.at[part, rows],
            share_sem, 2 * number + part, seq=toggled(q, bit),
        )

    def share_start(number, part):
        _, _, length, _, give, place = plans[part][number]
        weight_out[part, place : place + length] = weight_grad[
            rows_at(give, length), lanes_of(part)
        ].astype(BF16)
        share_copy(number, part).start()

    def share_finish(number, part):
        _, halves, length, keep, _, place = plans[part][number]
        with jax.named_scope("share_wait"):
            share_copy(number, part).wait()
        found = weight_in[part, place : place + length].astype(F32)
        if halves:
            kept = weight_grad[rows_at(keep, length), lanes_of(part)]
        else:
            kept = weight_out[part, place : place + length].astype(F32)
        weight_grad[rows_at(keep, length), lanes_of(part)] = kept + found

    def spread_copy(number, part, arrival=False):
        bit, _, length, keep, give, _ = plans[part][number]
        place = weight_all.at[rows_at(give if arrival else keep, length), lanes_of(part)]
        return remote(
            place, place, share_sem, 2 * (levels + number) + part, seq=toggled(q, bit)
        )

    def weight_event(stage, part):
        if stage < levels:
            share_finish(stage - 1, part)
            share_start(stage, part)
        elif stage == levels:
            share_finish(stage - 1, part)
            _, _, length, keep, _, _ = plans[part][-1]
            rows = rows_at(keep, length)
            weight_all[rows, lanes_of(part)] = weight_grad[rows, lanes_of(part)].astype(BF16)
            spread_copy(halvings[-1], part).start()
        else:
            number = halvings[levels - stage]
            with jax.named_scope("spread_wait"):
                spread_copy(number, part, arrival=True).wait_recv()
            if number > 0:
                spread_copy(number - 1, part).start()

    events = [(stage, 1 - part) for stage in range(1, levels + len(halvings) + 1) for part in range(2)]
    distance = groups_along - 1 - group
    far = distance >= 2
    ready_at = jnp.where(distance == 1, messages // 2, messages - 1)

    def weights_ready():
        for slot, peer in enumerate(peers):
            with jax.named_scope("column_wait"):
                column_arrival(slot, peer).wait_recv()
        with jax.named_scope("weight_dot"):
            weight_phase(columns, cotangents, weight_grad)
        share_start(0, 1)
        share_start(0, 0)

    def back_before(number):
        pl.when((number == 0) & far)(weights_ready)

    def back_step(number):
        chain_step(
            number, back_states, back_other, end_grad, back_sems,
            jnp.logical_not(odd), ends, begins, q - 2,
        )
        pl.when((number == ready_at) & jnp.logical_not(far))(weights_ready)
        for place, event in zip(CHAIN_HOOKS, events):
            pl.when((number == place) & far)(functools.partial(weight_event, *event))

    with jax.named_scope("inside_grad"):
        inside_grad_phase(
            act, cum_wide, dt_wide, cum_rows, scores, inside, scanned_grad, entering,
            scaled_grad, score_grad, query_grad, row_sums, back_before, back_step,
        )
    near = jnp.logical_not(far)

    def end_before(number):
        return_copy(back_other, end_grad, back_sems[2], number, arrival=True).wait_recv()

    def end_hook(index):
        for number in range(2):
            pl.when((index == NEAR_HOOKS[number]) & near)(
                functools.partial(weight_event, *events[number])
            )
            pl.when((index == FAR_HOOKS[number]) & far)(
                functools.partial(weight_event, *events[number + 2])
            )

    with jax.named_scope("end"):
        end_phase(
            act, slope, cum_wide, dt_wide, cum_cols, dt_cols, decay_wide, skip_wide, scanned_grad,
            scaled_grad, score_grad, query_grad, row_sums, entering, end_grad, key_grad, skip_sum,
            step, step_bias, decay_log, raw, halo, taps, window, filtered_grad,
            step_grad, filter_sums, head_sums, end_before, end_hook,
        )
    left = events[4:]
    heads_out[...] = filtered_grad[0:8, :]
    back_copy = remote(heads_out, following, halo_sem, 1, seq=q - 1)
    pl.when(jnp.logical_not(first))(back_copy.start)

    @pl.when(last)
    def _():
        following[...] = jnp.zeros_like(following)

    small[...] = filter_sums[...]
    small[count + 1 : count + 2, 0:inner] = norm_grad[0:1, :]
    for row in range(3):
        small[count + 2 : count + 3, row * LANES : (row + 1) * LANES] = head_sums[row : row + 1, :]

    steps = [("dp", bit) for bit in (1, 2)] + [("seq", bit) for bit in bits]

    def small_copy(number):
        axis, bit = steps[number]
        target = {"seq": toggled(q, bit)} if axis == "seq" else {"dp": toggled(d, bit)}
        return remote(small_in.at[2 * number], small_in.at[2 * number + 1], small_sem, number, **target)

    def small_start(number):
        small_in[2 * number] = small[...]
        small_copy(number).start()

    def small_step(number):
        with jax.named_scope("small_wait"):
            small_copy(number).wait()
        small[...] += small_in[2 * number + 1]
        if number + 1 < len(steps):
            small_start(number + 1)

    small_start(0)

    @pl.when(near)
    def _():
        weight_event(*events[2])
        weight_event(*events[3])

    small_step(0)
    pl.when(jnp.logical_not(last))(back_copy.wait_recv)
    with jax.named_scope("filter_grad"):
        filter_grad_phase(filtered_grad, following, taps, window, input_grad)
    number = 1
    while left or number < len(steps):
        for event in left[:2]:
            weight_event(*event)
        left = left[2:]
        if number < len(steps):
            small_step(number)
            number += 1

    store_weight = pltpu.make_async_copy(weight_all, weight_result, local_sem.at[1])
    store_weight.start()
    filter_out[...] = small[0 : count + 1, :]
    for index in range(inner // LANES):
        norm_out[index : index + 1, :] = small[
            count + 1 : count + 2, index * LANES : (index + 1) * LANES
        ]
    for row in range(3):
        head_out[row : row + 1, :] = small[
            count + 2 : count + 3, row * LANES : row * LANES + step.shape[0]
        ]
    for number in halvings:
        for part in range(2):
            spread_copy(number, part).wait_send()
    gather(d, 0, across).wait_send()
    gather(d, 1, beside).wait_send()
    gather(across, 2, beside).wait_send()
    for slot in (1, 2, 3):
        partial_copy(slot).wait_send()
    for slot, peer in enumerate(peers):
        column_copy(slot, peer).wait_send()
    pl.when(jnp.logical_not(last))(halo_copy.wait_send)
    pl.when(jnp.logical_not(first))(back_copy.wait_send)

    def drain(index, carry):
        chain_end(index, states, states_other, entering, ahead_sems, ends, q + 2)
        chain_end(index, back_states, back_other, end_grad, back_sems, begins, q - 2)
        return carry

    with jax.named_scope("drain"):
        lax.fori_loop(0, messages, drain, 0)
    store_gate.wait()
    store_weight.wait()


def body(
    conv_input,
    gate_input,
    step_input,
    filter_taps,
    filter_bias,
    step_bias,
    decay_log,
    skip_gain,
    norm_weight,
    output_weight,
    output_grad,
):
    raw, gate, step, cotangent = conv_input[0], gate_input[0], step_input[0], output_grad[0]
    tokens, channels = raw.shape
    inner = gate.shape[1]
    heads = step.shape[0]
    own_rows, width = output_weight.shape
    count = filter_taps.shape[0]
    spans, groups = lax.axis_size("seq"), lax.axis_size("dp")
    half = tokens // 2
    chunks = inner // LANES
    messages = chunks // 2
    assert groups == 4 and tokens % 256 == 0 and inner % (2 * LANES) == 0
    levels = spans.bit_length() - 1
    shared, size = 0, own_rows
    for _ in range(levels):
        size = size // 2 if size // 2 % 16 == 0 else size
        shared += size
    wide = pltpu.VMEM((tokens, inner), F32)
    full = pltpu.VMEM((tokens, channels), F32)
    columns = pltpu.VMEM((tokens, LANES), F32)
    row8 = pltpu.VMEM((8, inner), F32)
    stored = pltpu.VMEM((chunks, LANES, LANES), F32)
    turned = pltpu.VMEM((2, LANES, tokens), BF16)
    squares = pltpu.VMEM((3, half, half), F32)
    edge = pltpu.VMEM((8, channels), F32)
    sems = pltpu.SemaphoreType.DMA
    scratch = [
        pltpu.VMEM((tokens, inner), BF16), pltpu.VMEM((tokens, inner), BF16),
        pltpu.VMEM((own_rows, width), F32), edge, row8,
        pltpu.VMEM((16, channels), BF16),
        pltpu.VMEM((own_rows, width), BF16),
        pltpu.VMEM((groups, tokens, width), BF16),
        full, full, wide, wide, row8, row8,
        pltpu.VMEM((heads, 1, tokens), F32), columns, columns, turned, turned,
        pltpu.VMEM((2, tokens + 8, LANES), F32), squares,
        stored, stored, stored, wide, wide, columns,
        pltpu.VMEM((groups, tokens, own_rows), BF16),
        pltpu.VMEM((groups, tokens, own_rows), BF16),
        pltpu.VMEM((groups, tokens, own_rows), F32),
        pltpu.VMEM((groups, tokens, own_rows), BF16),
        pltpu.VMEM((tokens, own_rows), F32),
        pltpu.VMEM((2, tokens, own_rows), BF16),
        wide, wide, row8, row8,
        stored, stored, stored, squares, columns, columns, columns,
        edge, pltpu.VMEM((8, LANES), F32), edge, edge,
        pltpu.VMEM((2, shared, width // 2), BF16),
        pltpu.VMEM((2, shared, width // 2), BF16),
        pltpu.VMEM((own_rows, width), BF16),
        pltpu.VMEM((2 * (levels + 2), 8, channels), F32),
        sems((3,)), sems((2, 2)), sems((2, 1)), sems((2, 3)), sems((2, 3)), sems((2, 3)),
        sems((2, messages)), sems((2, messages)), sems((2, 2, messages)), sems((2, 2, messages)),
        sems((2, 4 * levels)), sems((2, levels + 2)),
    ]
    outs = [
        ((tokens, channels), BF16), ((tokens, inner), BF16), ((heads, tokens), F32),
        ((own_rows, width), BF16), ((count + 1, channels), F32), ((chunks, LANES), F32),
        ((3, heads), F32),
    ]
    args = (
        raw, step, filter_taps, filter_bias.reshape(channels // LANES, LANES),
        step_bias[None], decay_log[None], skip_gain[None],
        norm_weight.reshape(chunks, LANES), output_weight, cotangent, gate,
    )
    vmem = pl.BlockSpec(memory_space=pltpu.VMEM)
    anywhere = pl.BlockSpec(memory_space=pl.ANY)
    results = pl.pallas_call(
        functools.partial(layer_kernel, spans, groups),
        out_shape=[jax.ShapeDtypeStruct(shape, kind) for shape, kind in outs],
        in_specs=[vmem] * (len(args) - 3) + [anywhere] * 3,
        out_specs=[vmem, anywhere, vmem, anywhere, vmem, vmem, vmem],
        scratch_shapes=scratch,
        compiler_params=pltpu.CompilerParams(
            vmem_limit_bytes=67043328, has_side_effects=True, collective_id=0
        ),
    )(*args)
    kinds = [outs[number] for number in range(len(outs))]
    kinds[3] = ((own_rows, width), F32)
    input_grad, gate_grad, step_grad, weight_grad, filter_grads, norm_grad, head_grads = pl.pallas_call(
        finish_kernel,
        out_shape=[jax.ShapeDtypeStruct(shape, kind) for shape, kind in kinds],
        in_specs=[anywhere] * len(outs),
        out_specs=[anywhere] * len(outs),
        scratch_shapes=[pltpu.VMEM(*out) for out in outs]
        + [pltpu.VMEM(*kinds[3]), sems((len(outs),)), sems((len(outs),))],
        compiler_params=pltpu.CompilerParams(vmem_limit_bytes=67043328),
    )(*results)
    return (
        input_grad[None], gate_grad[None], step_grad[None], weight_grad,
        filter_grads, norm_grad.reshape(inner), head_grads,
    )


def finish_kernel(*refs):
    count = (len(refs) - 3) // 3
    sources, targets, held = refs[:count], refs[count : 2 * count], list(refs[2 * count : 3 * count])
    widened, load_sem, store_sem = refs[3 * count :]
    loads = [
        pltpu.make_async_copy(source, buffer, load_sem.at[number])
        for number, (source, buffer) in enumerate(zip(sources, held))
    ]
    order = [3] + [number for number in range(count) if number != 3]
    for number in order:
        loads[number].start()
    stores = []
    for number in order:
        loads[number].wait()
        buffer = held[number]
        if number == 3:
            widened[...] = buffer[...].astype(F32)
            buffer = widened
        store = pltpu.make_async_copy(buffer, targets[number], store_sem.at[number])
        store.start()
        stores.append(store)
    for store in stores:
        store.wait()


def solution(mesh):
    return jax.shard_map(
        body,
        mesh=mesh,
        in_specs=(
            P("dp", "seq", None),
            P("dp", "seq", None),
            P("dp", None, "seq"),
            P(),
            P(),
            P(),
            P(),
            P(),
            P(),
            P("dp", None),
            P("dp", "seq", None),
        ),
        out_specs=(
            P("dp", "seq", None),
            P("dp", "seq", None),
            P("dp", None, "seq"),
            P("dp", None),
            P(),
            P(),
            P(),
        ),
        check_vma=False,
    )
```

```python
import functools

import jax
import jax.numpy as jnp
from jax import lax
from jax.experimental import pallas as pl
from jax.experimental.pallas import tpu as pltpu
from jax.sharding import PartitionSpec as P

F32 = jnp.float32
BF16 = jnp.bfloat16
EPSILON = 1e-05
LOG2E = 1.4426950408889634
LANES = 128
HEAD_DIM = 64
MESH = pl.DeviceIdType.MESH
CHAIN_HOOKS = (6, 6, 9, 9)
FAR_HOOKS = (4, 4, 8, 8)
NEAR_HOOKS = (6, 6, 9, 9)
NN = (((1,), (0,)), ((), ()))
NT = (((1,), (1,)), ((), ()))
TN = (((0,), (0,)), ((), ()))


def dot(a, b, dims=NN):
    return lax.dot_general(a, b, dims, preferred_element_type=F32)


def rounded_high(a):
    scaled = a * 65537.0
    return scaled - (scaled - a)


def split2(a):
    high = rounded_high(a)
    return high.astype(BF16), (a - high).astype(BF16)


def split3(a):
    high = rounded_high(a)
    rest = a - high
    middle = rounded_high(rest)
    return high.astype(BF16), middle.astype(BF16), (rest - middle).astype(BF16)


def dot3(a, b, dims=NN):
    return dot(a[0], b[0], dims) + (dot(a[0], b[1], dims) + dot(a[1], b[0], dims))


def chunk_of(index):
    return pl.ds(pl.multiple_of(index * LANES, LANES), LANES)


def iota(shape, dim):
    return lax.broadcasted_iota(jnp.int32, shape, dim)


def low_half(shape):
    return iota(shape, 1) < HEAD_DIM


def head_rows(index):
    shape = (LANES, LANES)
    wanted = 2 * index + jnp.where(low_half(shape), 0, 1)
    return jnp.where(iota(shape, 0) == wanted, 1.0, 0.0).astype(BF16)


def sigmoid(a):
    return 1.0 / (1.0 + jnp.exp(-a))


def transposed(rows):
    heads, tokens = rows.shape
    padded = jnp.concatenate([rows, jnp.zeros((LANES - heads, tokens), F32)], axis=0)
    return padded.T


def padded_row(row):
    short = row[...]
    return jnp.concatenate([short, jnp.zeros((1, LANES - short.shape[1]), F32)], axis=1)


def column_of(row):
    return jnp.broadcast_to(padded_row(row), (LANES, LANES)).T[: row.shape[1], 0:1]


def step_phase(step, step_bias, decay_log, cum_rows, cum_cols, dt_cols):
    shifted = step[...] + column_of(step_bias)
    sizes = jnp.maximum(shifted, 0.0) + jnp.log1p(jnp.exp(-jnp.abs(shifted)))
    rates = -jnp.exp(column_of(decay_log)) * sizes
    tokens = rates.shape[1]
    shape = (tokens, tokens)
    before = jnp.where(iota(shape, 0) <= iota(shape, 1), 1.0, 0.0).astype(BF16)
    high, middle, low = split3(rates)
    cumulative = (dot(high, before) + (dot(middle, before) + dot(low, before))) * LOG2E
    for head in range(rates.shape[0]):
        cum_rows[head] = cumulative[head : head + 1]
    cum_cols[...] = transposed(cumulative)
    dt_cols[...] = transposed(sizes)


def expand_phase(cum_cols, dt_cols, skip_gain, cum_wide, dt_wide, decay_wide, skip_wide):
    tokens, inner = cum_wide.shape
    cum_parts = split3(cum_cols[...])
    dt_parts = split3(dt_cols[...])
    skip_parts = split3(jnp.broadcast_to(padded_row(skip_gain), (8, LANES)))

    def each(index, carry):
        here = chunk_of(index)
        rows = head_rows(index)
        wide = dot(cum_parts[0], rows) + (dot(cum_parts[1], rows) + dot(cum_parts[2], rows))
        cum_wide[:, here] = wide
        skip_wide[:, here] = dot(skip_parts[0], rows) + (
            dot(skip_parts[1], rows) + dot(skip_parts[2], rows)
        )
        dt_wide[:, here] = dot(dt_parts[0], rows) + (
            dot(dt_parts[1], rows) + dot(dt_parts[2], rows)
        )
        decay_wide[:, here] = jnp.broadcast_to(jnp.exp2(wide[tokens - 1 : tokens]), (8, LANES))
        return carry

    lax.fori_loop(0, inner // LANES, each, 0, unroll=4)


def filter_chunk(index, slot, here, raw, halo, taps, bias, windows, act, slope):
    tokens = raw.shape[0]
    window = windows.at[slot]
    window[0:8, :] = halo[:, here].astype(F32)[8:]
    window[8 : 8 + tokens, :] = raw[:, here].astype(F32)
    count = taps.shape[0]
    filtered = bias[pl.ds(index, 1), :] + taps[0:1, here] * window[9 - count : 9 - count + tokens, :]
    for k in range(1, count):
        filtered = filtered + taps[k : k + 1, here] * window[9 - count + k : 9 - count + k + tokens, :]
    gate = sigmoid(filtered)
    result = filtered * gate
    act[:, here] = result
    slope[:, here] = gate + result * (1.0 - gate)
    return result


def in_pairs(total, before, after, each, carry):
    def several(number, carry):
        if before is not None:
            before(number)
        for j in range(2):
            carry = each(2 * number + j, carry, j)
        if after is not None:
            after(number)
        return carry

    return lax.fori_loop(0, total // 2, several, carry)


def state_phase(
    raw, halo, taps, bias, window, act, slope, cum_wide, dt_wide, key_t, query_t, states, after
):
    tokens, inner = cum_wide.shape
    first = inner // LANES
    key = filter_chunk(first, 0, pl.ds(inner, LANES), raw, halo, taps, bias, window, act, slope)
    query = filter_chunk(first + 1, 1, pl.ds(inner + LANES, LANES), raw, halo, taps, bias, window, act, slope)
    high, low = split2(key.T)
    key_t[0], key_t[1] = high, low
    high, low = split2(query.T)
    query_t[0], query_t[1] = high, low

    def each(index, carry, slot):
        here = chunk_of(index)
        values = filter_chunk(index, slot, here, raw, halo, taps, bias, window, act, slope)
        cum = cum_wide[:, here]
        moved = values * dt_wide[:, here] * jnp.exp2(cum[tokens - 1 : tokens] - cum)
        states[index] = dot3((key_t[0], key_t[1]), split2(moved))
        return carry

    in_pairs(first, None, after, each, 0)


def score_blocks(act, inner, scores):
    half = act.shape[0] // 2
    key = split2(act[:, inner : inner + LANES])
    query = split2(act[:, inner + LANES : inner + 2 * LANES])
    shape = (half, half)
    causal = iota(shape, 0) >= iota(shape, 1)
    for slot, (rows, columns) in enumerate(((0, 0), (1, 1), (1, 0))):
        left = tuple(part[rows * half : (rows + 1) * half] for part in query)
        right = tuple(part[columns * half : (columns + 1) * half] for part in key)
        block = dot3(left, right, NT)
        if rows == columns:
            block = jnp.where(causal, block, 0.0)
        scores[slot] = block


def decay_blocks(index, cum, cum_rows, half, block):
    rows = slice(block * half, (block + 1) * half)
    found = []
    for j in range(2):
        column = jnp.broadcast_to(cum[rows, j * HEAD_DIM : j * HEAD_DIM + 1], (half, half))
        row = cum_rows[2 * index + j][:, rows]
        found.append(jnp.exp2(jnp.minimum(column - row, 0.0)))
    return jnp.concatenate(found, axis=1)


def stacked(block):
    low = low_half(block.shape)
    zero = jnp.zeros_like(block)
    return jnp.concatenate([jnp.where(low, block, zero), jnp.where(low, zero, block)], axis=0)


def inside_phase(act, cum_wide, dt_wide, cum_rows, scores, inside, before, after):
    tokens, inner = cum_wide.shape
    half = tokens // 2

    def each(index, carry, slot):
        here = chunk_of(index)
        scaled = act[:, here] * dt_wide[:, here]
        cum = cum_wide[:, here]
        for block in range(2):
            rows = slice(block * half, (block + 1) * half)
            weights = decay_blocks(index, cum, cum_rows, half, block)
            score = scores[block]
            weights = jnp.concatenate([score, score], axis=1) * weights
            right = stacked(scaled[rows])
            result = dot3(split2(weights), split2(right))
            if block == 1:
                middle = cum[half - 1 : half]
                moved = scaled[:half] * jnp.exp2(middle - cum[:half])
                result = result + jnp.exp2(cum[half:] - middle) * dot3(
                    split2(scores[2]), split2(moved)
                )
            inside[rows, here] = result
        return carry

    in_pairs(inner // LANES, before, after, each, 0)


def norm_phase(act, cum_wide, inside, entering, skip_wide, gate, norm_weight, gated, scale, low):
    tokens, inner = cum_wide.shape
    query = split2(act[:, inner + LANES : inner + 2 * LANES])

    def each(index, total):
        here = chunk_of(index)
        crossed = jnp.exp2(cum_wide[:, here]) * dot3(query, split2(entering[index]))
        scanned = inside[:, here] + crossed
        inside[:, here] = scanned
        scanned = scanned + skip_wide[0:1, here] * act[:, here]
        branch = gate[:, here].astype(F32)
        result = scanned * (branch * sigmoid(branch))
        gated[:, here] = result
        return total + result * result

    total = lax.fori_loop(0, inner // LANES, each, jnp.zeros((tokens, LANES), F32), unroll=2)
    mean = jnp.sum(total, axis=1, keepdims=True) / inner
    inverse = lax.rsqrt(mean + EPSILON)
    scale[...] = jnp.broadcast_to(inverse, scale.shape)

    per = low.shape[2] // LANES

    def rounded(index, carry):
        here = chunk_of(index)
        place = pl.ds(pl.multiple_of(index % per * LANES, LANES), LANES)
        result = gated[:, here] * scale[...] * norm_weight[pl.ds(index, 1), :]
        low[index // per, :, place] = result.astype(BF16)
        return carry

    lax.fori_loop(0, inner // LANES, rounded, 0)


def gate_phase(
    act, cum_wide, inside, skip_wide, gate, norm_weight, gated, scale, query_t,
    chip, normed_sent, normed_grad, scanned_grad, gate_grad, norm_grad, skip_sum, entering_grad,
    after,
):
    tokens, inner = cum_wide.shape

    per = normed_grad.shape[2] // LANES

    def normed_at(index):
        return normed_grad[index // per, :, chunk_of(index % per)]

    def first(index, total):
        here = chunk_of(index)
        slot, place = index // per, chunk_of(index % per)
        sent = normed_sent[slot, :, place].astype(F32)
        found = jnp.where(slot // 2 == chip, normed_grad[slot, :, place], sent)
        normed_grad[slot, :, place] = found
        return total + found * norm_weight[pl.ds(index, 1), :] * gated[:, here]

    total = lax.fori_loop(0, inner // LANES, first, jnp.zeros((tokens, LANES), F32), unroll=2)
    inverse = scale[...]
    pull = jnp.sum(total, axis=1, keepdims=True) / inner * inverse * inverse * inverse

    def second(index, carry, slot):
        here = chunk_of(index)
        found = normed_at(index)
        product = gated[:, here]
        norm_grad[:, here] = jnp.broadcast_to(
            jnp.sum(found * product * inverse, axis=0, keepdims=True), (8, LANES)
        )
        down = inverse * (found * norm_weight[pl.ds(index, 1), :]) - product * pull
        branch = gate[:, here].astype(F32)
        opened = sigmoid(branch)
        passed = branch * opened
        values = act[:, here]
        scanned = inside[:, here] + skip_wide[0:1, here] * values
        gate_grad[:, here] = (down * scanned * (opened + passed * (1.0 - opened))).astype(BF16)
        back = down * passed
        scanned_grad[:, here] = back
        skip_sum[:, here] = jnp.broadcast_to(
            jnp.sum(back * values, axis=0, keepdims=True), (8, LANES)
        )
        moved = back * jnp.exp2(cum_wide[:, here])
        entering_grad[index] = dot3((query_t[0], query_t[1]), split2(moved))
        return carry

    in_pairs(inner // LANES, None, after, second, 0)


def inside_grad_phase(
    act, cum_wide, dt_wide, cum_rows, scores, inside, scanned_grad, entering,
    scaled_grad, score_grad, query_grad, row_sums, before, after,
):
    tokens, inner = cum_wide.shape
    half = tokens // 2
    score_grad[...] = jnp.zeros_like(score_grad)
    query_grad[...] = jnp.zeros_like(query_grad)
    row_sums[...] = jnp.zeros_like(row_sums)

    def each(index, carry, slot):
        here = chunk_of(index)
        scaled = act[:, here] * dt_wide[:, here]
        cum = cum_wide[:, here]
        back = scanned_grad[:, here]
        middle = cum[half - 1 : half]
        for block in range(2):
            rows = slice(block * half, (block + 1) * half)
            decay = decay_blocks(index, cum, cum_rows, half, block)
            score = scores[block]
            weights = split2(jnp.concatenate([score, score], axis=1) * decay)
            down = split2(back[rows])
            products = dot3(down, split2(stacked(scaled[rows])), NT) * decay
            score_grad[block] += products[:, :half] + products[:, half:]
            found = dot3(weights, down, TN)
            found = jnp.where(low_half((half, LANES)), found[:half], found[half:])
            if block == 0:
                pulled = split2(back[half:] * jnp.exp2(cum[half:] - middle))
                factor = jnp.exp2(middle - cum[:half])
                score_grad[2] += dot3(pulled, split2(scaled[:half] * factor), NT)
                found = found + factor * dot3(split2(scores[2]), pulled, TN)
            scaled_grad[rows, here] = found
        query_grad[...] += dot3(split2(back * jnp.exp2(cum)), split2(entering[index]), NT)
        rows = head_rows(index)
        high, low = split2(back * inside[:, here])
        row_sums[...] += dot(high, rows, NT) + dot(low, rows, NT)
        return carry

    in_pairs(inner // LANES, before, after, each, 0)


def end_phase(
    act, slope, cum_wide, dt_wide, cum_cols, dt_cols, decay_wide, skip_wide, scanned_grad,
    scaled_grad, score_grad, query_grad, row_sums, entering, end_grad, key_grad, skip_sum,
    step, step_bias, decay_log, raw, halo, taps, windows, filtered_grad,
    step_grad, filter_sums, head_sums, before_pair, after_pair,
):
    tokens, inner = cum_wide.shape
    half = tokens // 2
    key = split2(act[:, inner : inner + LANES])
    query = split2(act[:, inner + LANES : inner + 2 * LANES])
    count = taps.shape[0]

    def finish(slot, here, found):
        pulled = found * slope[:, here]
        filtered_grad[:, here] = pulled
        window = windows.at[slot]
        window[0:8, :] = halo[:, here].astype(F32)[8:]
        window[8 : 8 + tokens, :] = raw[:, here].astype(F32)
        sums = [
            jnp.sum(pulled * window[9 - count + k : 9 - count + k + tokens, :], axis=0, keepdims=True)
            for k in range(count)
        ]
        sums.append(jnp.sum(pulled, axis=0, keepdims=True))
        sums.append(jnp.zeros((8 - len(sums), LANES), F32))
        filter_sums[:, here] = jnp.concatenate(sums, axis=0)

    key_grad[...] = jnp.zeros_like(key_grad)
    zeros = (jnp.zeros((tokens, LANES), F32), jnp.zeros((8, LANES), F32), jnp.zeros((8, LANES), F32))

    def each(index, sums, slot):
        value_sums, last_sums, skip_sums = sums
        here = chunk_of(index)
        values = act[:, here]
        sizes = dt_wide[:, here]
        cum = cum_wide[:, here]
        to_end = jnp.exp2(cum[tokens - 1 : tokens] - cum)
        after = end_grad[index]
        parts = split2(after)
        moved = values * sizes * to_end
        moved_grad = dot3(key, parts)
        key_grad[...] += dot3(split2(moved), parts, NT)
        last = jnp.sum(moved * moved_grad, axis=0, keepdims=True) + decay_wide[0:1, here] * jnp.sum(
            after * entering[index], axis=0, keepdims=True
        )
        scaled = scaled_grad[:, here] + to_end * moved_grad
        rows = head_rows(index)
        high, low = split2(scaled * values)
        value_sums = value_sums + (dot(high, rows, NT) + dot(low, rows, NT))
        parts = split3(jnp.broadcast_to(last, (8, LANES)))
        last_sums = last_sums + (dot(parts[0], rows, NT) + (dot(parts[1], rows, NT) + dot(parts[2], rows, NT)))
        parts = split3(skip_sum[:, here])
        skip_sums = skip_sums + (dot(parts[0], rows, NT) + (dot(parts[1], rows, NT) + dot(parts[2], rows, NT)))
        finish(slot, here, scaled * sizes + skip_wide[0:1, here] * scanned_grad[:, here])
        return value_sums, last_sums, skip_sums

    value_sums, last_sums, skip_sums = in_pairs(inner // LANES, before_pair, after_pair, each, zeros)

    shape = (half, half)
    causal = iota(shape, 0) >= iota(shape, 1)
    blocks = [split2(jnp.where(causal, score_grad[slot], 0.0)) for slot in range(2)]
    blocks.append(split2(score_grad[2]))
    first = lambda parts: tuple(part[:half] for part in parts)
    second = lambda parts: tuple(part[half:] for part in parts)
    upper = dot3(blocks[0], first(key))
    lower = dot3(blocks[1], second(key)) + dot3(blocks[2], first(key))
    finish(1, pl.ds(inner + LANES, LANES), query_grad[...] + jnp.concatenate([upper, lower], axis=0))
    upper = dot3(blocks[0], first(query), TN) + dot3(blocks[2], second(query), TN)
    lower = dot3(blocks[1], second(query), TN)
    finish(0, pl.ds(inner, LANES), key_grad[...] + jnp.concatenate([upper, lower], axis=0))

    sizes = dt_cols[...]
    cum_grad = row_sums[...] - sizes * value_sums
    at_end = iota((tokens, LANES), 0) == tokens - 1
    cum_grad = cum_grad + jnp.where(at_end, jnp.broadcast_to(last_sums[0:1], (tokens, LANES)), 0.0)
    shape = (tokens, tokens)
    after = jnp.where(iota(shape, 0) <= iota(shape, 1), 1.0, 0.0).astype(BF16)
    parts = split3(cum_grad)
    rate_grad = dot(after, parts[0]) + (dot(after, parts[1]) + dot(after, parts[2]))
    rate = -jnp.exp(padded_row(decay_log))
    heads = step.shape[0]
    shifted = transposed(step[...] + column_of(step_bias))
    pulled = (value_sums + rate_grad * rate) * sigmoid(shifted)
    pulled = jnp.where(iota((tokens, LANES), 1) < heads, pulled, 0.0)
    step_grad[...] = pulled.T[:heads]
    head_sums[...] = jnp.concatenate(
        [
            jnp.sum(pulled, axis=0, keepdims=True),
            jnp.sum(rate_grad * rate * sizes, axis=0, keepdims=True),
            skip_sums[0:1],
            jnp.zeros((5, LANES), F32),
        ],
        axis=0,
    )


def filter_grad_phase(filtered_grad, following, taps, windows, input_grad):
    tokens, channels = filtered_grad.shape
    count = taps.shape[0]

    def each(index, carry, slot):
        here = chunk_of(index)
        window = windows.at[slot]
        window[0:tokens, :] = filtered_grad[:, here]
        window[tokens : tokens + 8, :] = following[:, here]
        total = taps[count - 1 : count, here] * window[0:tokens, :]
        for k in range(count - 1):
            offset = count - 1 - k
            total = total + taps[k : k + 1, here] * window[offset : offset + tokens, :]
        input_grad[:, here] = total.astype(BF16)
        return carry

    in_pairs(channels // LANES, None, None, each, 0)


def toggled(index, bit):
    return index + bit - 2 * bit * (index // bit % 2)


def weight_phase(columns, cotangents, total):
    peers, tokens, rows = columns.shape

    def each(index, carry):
        here = chunk_of(index)
        found = dot(columns[0, :, here], cotangents[0], TN)
        for peer in range(1, peers):
            found = found + dot(columns[peer, :, here], cotangents[peer], TN)
        total[pl.ds(pl.multiple_of(index * LANES, LANES), LANES), :] = found
        return carry

    lax.fori_loop(0, rows // LANES, each, 0)


def layer_kernel(
    spans, groups,
    raw, step, taps, bias, step_bias, decay_log, skip_gain, norm_weight,
    weight, cotangent, gate_in,
    input_grad, gate_out, step_grad, weight_result, filter_out, norm_out, head_out,
    gate, gate_grad, weight_grad, small, skip_wide, halo, weights, cotangents, act, slope, cum_wide, dt_wide, decay_wide, other_decay,
    cum_rows, cum_cols, dt_cols, key_t, query_t, window, scores,
    states, states_other, entering, inside, gated, scale, low, columns,
    normed_grad, normed_sent, partial_beside, partials, scaled_grad, scanned_grad, norm_grad, skip_sum,
    back_states, back_other, end_grad, score_grad, query_grad, row_sums, key_grad,
    filter_sums, head_sums, following, heads_out,
    weight_out, weight_in, weight_all, small_in,
    local_sem, halo_sem, decay_sem, gather_sem, partial_sem, column_sem, ahead_sem, back_sem, next_sem, return_sem,
    share_sem, small_sem,
):
    q, d = lax.axis_index("seq"), lax.axis_index("dp")
    tokens, channels = raw.shape
    inner = gate_in.shape[1]
    own_rows = weight.shape[0]
    count = taps.shape[0]
    filtered_grad = act

    def remote(source, target, sems, slot, seq=None, dp=None):
        return pltpu.make_async_remote_copy(
            src_ref=source,
            dst_ref=target,
            send_sem=sems.at[0, slot],
            recv_sem=sems.at[1, slot],
            device_id=(q if seq is None else seq, d if dp is None else dp),
            device_id_type=MESH,
        )

    first, last = q == 0, q == spans - 1
    partner = toggled(q, 1)
    odd = q % 2 == 1
    group, groups_along = q // 2, spans // 2

    load_weight = pltpu.make_async_copy(weight, weights, local_sem.at[0])
    load_cotangent = pltpu.make_async_copy(cotangent, cotangents.at[d], local_sem.at[1])
    load_gate = pltpu.make_async_copy(gate_in, gate, local_sem.at[2])
    load_cotangent.start()
    load_weight.start()
    load_gate.start()

    across, beside = toggled(d, 2), toggled(d, 1)
    bits = []
    while 2 ** len(bits) < spans:
        bits.append(2 ** len(bits))
    barrier = pltpu.get_barrier_semaphore()

    def greet(seq, dp):
        pl.semaphore_signal(barrier, inc=1, device_id=(seq, dp), device_id_type=MESH)

    for other in (across, beside, toggled(across, 1)):
        greet(q, other)
    for bit in bits:
        greet(toggled(q, bit), d)
    expected = 3 + len(bits)
    for distance in (1, 2):
        below, above = q >= distance, q < spans - distance
        pl.when(below)(lambda distance=distance: greet(q - distance, d))
        pl.when(above)(lambda distance=distance: greet(q + distance, d))
        expected = expected + jnp.where(below, 1, 0) + jnp.where(above, 1, 0)

    with jax.named_scope("steps"):
        step_phase(step, step_bias, decay_log, cum_rows, cum_cols, dt_cols)
    with jax.named_scope("barrier"):
        pl.semaphore_wait(barrier, expected)

    with jax.named_scope("halo_start"):
        halo_copy = remote(raw.at[tokens - 16 : tokens], halo, halo_sem, 0, seq=q + 1)
    pl.when(jnp.logical_not(last))(halo_copy.start)

    @pl.when(first)
    def _():
        halo[...] = jnp.zeros_like(halo)

    diagonal = toggled(across, 1)

    def gather(owner, slot, target):
        place = cotangents.at[owner]
        return remote(place, place, gather_sem, slot, dp=target)

    load_cotangent.wait()
    gather(d, 0, across).start()
    gather(d, 1, beside).start()

    with jax.named_scope("expand"):
        expand_phase(cum_cols, dt_cols, skip_gain, cum_wide, dt_wide, decay_wide, skip_wide)
    decay_copy = remote(decay_wide, other_decay, decay_sem, 0, seq=partner)
    decay_copy.start()
    pl.when(jnp.logical_not(first))(halo_copy.wait_recv)

    side = q % 2

    def pair_copy(source, target, sems, number, arrival=False):
        at = 2 * number + (side if arrival else 1 - side)
        return remote(source.at[at], target.at[at], sems, number, seq=partner)

    with jax.named_scope("states"):
        state_phase(
            raw, halo, taps, bias, window, act, slope, cum_wide, dt_wide, key_t, query_t, states,
            lambda number: pair_copy(states, states_other, ahead_sem, number).start(),
        )
    with jax.named_scope("decay"):
        decay_copy.wait()
    score_blocks(act, inner, scores)

    def chain_copy(own, arrived, sems, number, towards):
        at = 2 * number + side
        return remote(own.at[at], arrived.at[at], sems, number, seq=towards)

    def return_copy(other, arrived, sems, number, arrival=False):
        at = 2 * number + (1 - side if arrival else side)
        return remote(other.at[at], arrived.at[at], sems, number, seq=partner)

    def chain_step(number, own, other, arrived, sems, late, begins, ends, towards):
        pair_sem, chain_sem, return_sem = sems
        chain = chain_copy(own, arrived, chain_sem, number, towards)
        with jax.named_scope("pair_wait"):
            pair_copy(own, other, pair_sem, number, arrival=True).wait_recv()
        with jax.named_scope("chain_wait"):
            pl.when(jnp.logical_not(begins))(chain.wait_recv)
        at = 2 * number + side
        here = chunk_of(at)
        mine, theirs = own[at], other[at]
        mine_decay, their_decay = decay_wide[0:1, here], other_decay[0:1, here]
        running = jnp.where(begins, 0.0, arrived[at])
        both = jnp.where(late, mine_decay * theirs + mine, their_decay * mine + theirs)
        own[at] = mine_decay * their_decay * running + both
        pl.when(jnp.logical_not(ends))(chain.start)
        arrived[at] = jnp.where(late, theirs + their_decay * running, running)
        other[at] = jnp.where(late, running, mine + mine_decay * running)
        return_copy(other, arrived, return_sem, number).start()

    def chain_end(number, own, other, arrived, sems, ends, towards):
        pair_sem, chain_sem, return_sem = sems
        pair_copy(own, other, pair_sem, number).wait_send()
        chain = chain_copy(own, arrived, chain_sem, number, towards)
        pl.when(jnp.logical_not(ends))(chain.wait_send)
        return_copy(other, arrived, return_sem, number).wait_send()

    messages = states.shape[0] // 2
    ahead_sems = (ahead_sem, next_sem.at[0], return_sem.at[0])
    back_sems = (back_sem, next_sem.at[1], return_sem.at[1])
    begins, ends = group == 0, group == groups_along - 1

    per_slot = own_rows // LANES
    owners = (d, beside, across, diagonal)
    load_weight.wait()

    def partial_copy(slot, arrival=False):
        owner = owners[slot]
        lands = owner if arrival else d
        if slot == 1:
            return remote(partial_beside, normed_grad.at[lands], partial_sem, 0, dp=owner)
        return remote(partials.at[slot - 2], normed_sent.at[lands], partial_sem, slot - 1, dp=owner)

    def partial_chunk(number):
        slot = number // per_slot
        owner = owners[3]
        for other in (2, 1, 0):
            owner = jnp.where(slot == other, owners[other], owner)
        index = number % per_slot
        rows = weights[pl.ds(pl.multiple_of(index * LANES, LANES), LANES), :]
        found = dot(cotangents[owner], rows, NT)

        @pl.when(slot == 0)
        def _():
            normed_grad[d, :, chunk_of(index)] = found

        @pl.when(slot == 1)
        def _():
            partial_beside[:, chunk_of(index)] = found

        @pl.when(slot > 1)
        def _():
            partials[slot - 2, :, chunk_of(index)] = found.astype(BF16)

        for slot in (1, 2, 3):
            pl.when(number == (slot + 1) * per_slot - 1)(partial_copy(slot).start)

    early = group < 2

    def across_arrives():
        gather(across, 0, across).wait_recv()
        gather(across, 2, beside).start()

    def partial_slots(first, last):
        def each(at, carry):
            partial_chunk(at)
            return carry

        lax.fori_loop(first * per_slot, last * per_slot, each, 0)

    def ahead_before(number):
        @pl.when((number == 0) & jnp.logical_not(early))
        def _():
            gather(beside, 1, beside).wait_recv()
            partial_slots(0, 2)
            across_arrives()
            partial_slots(2, 3)
            gather(diagonal, 2, beside).wait_recv()
            partial_slots(3, 4)

    def ahead_step(number):
        chain_step(
            number, states, states_other, entering, ahead_sems, odd, begins, ends, q + 2
        )

        pl.when(early & (number == per_slot))(across_arrives)
        pl.when(early & (number == per_slot + per_slot // 2))(gather(diagonal, 2, beside).wait_recv)

        @pl.when(early & (number >= per_slot))
        def _():
            for j in range(2):
                partial_chunk(2 * number + j)

    with jax.named_scope("inside"):
        inside_phase(
            act, cum_wide, dt_wide, cum_rows, scores, inside, ahead_before, ahead_step,
        )

    @pl.when(early)
    def _():
        gather(beside, 1, beside).wait_recv()
        partial_slots(0, 2)

    with jax.named_scope("return_wait"):
        for number in range(messages):
            return_copy(states_other, entering, ahead_sems[2], number, arrival=True).wait_recv()
    load_gate.wait()
    with jax.named_scope("norm"):
        norm_phase(act, cum_wide, inside, entering, skip_wide, gate, norm_weight, gated, scale, low)

    def column_copy(slot, peer):
        return remote(low.at[peer], columns.at[d], column_sem, slot, dp=peer)

    def column_arrival(slot, peer):
        return remote(low.at[peer], columns.at[peer], column_sem, slot, dp=peer)

    peers = (across, diagonal, beside)
    for slot, peer in enumerate(peers):
        column_copy(slot, peer).start()
    columns[d] = low[d]
    with jax.named_scope("partial_wait"):
        for slot in (1, 2, 3):
            partial_copy(slot, arrival=True).wait_recv()

    with jax.named_scope("gate"):
        gate_phase(
            act, cum_wide, inside, skip_wide, gate, norm_weight, gated, scale, query_t,
            d // 2, normed_sent, normed_grad, scanned_grad, gate_grad, norm_grad, skip_sum,
            back_states,
            lambda number: pair_copy(back_states, back_other, back_sem, number).start(),
        )

    store_gate = pltpu.make_async_copy(gate_grad, gate_out, local_sem.at[0])
    store_gate.start()

    def plan_for(order):
        size, base, offset = own_rows, 0, 0
        plan = []
        for bit in order:
            mine = q // bit % 2
            halves = size // 2 % 16 == 0
            if halves:
                size = size // 2
                keep, give = base + mine * size, base + (1 - mine) * size
                base = keep
            else:
                keep, give = base, base
            plan.append((bit, halves, size, keep, give, offset))
            offset = offset + size
        return plan

    plans = (plan_for(bits), plan_for(bits[1:] + bits[:1])) * 2
    levels = len(bits)
    halvings = [number for number in range(levels) if plans[0][number][1]]
    tiles = cotangent.shape[1] // LANES
    parts = 4
    edges = [-(-tiles * part // parts) * LANES for part in range(parts + 1)]
    order = (1, 3, 0, 2)

    def rows_at(start, length):
        return pl.ds(pl.multiple_of(start, 16), length)

    def lanes_of(part):
        return pl.ds(edges[part], edges[part + 1] - edges[part])

    def share_copy(number, part):
        bit, _, length, _, _, place = plans[part][number]
        rows = pl.ds(place, length)
        return remote(
            weight_out.at[rows, lanes_of(part)], weight_in.at[rows, lanes_of(part)],
            share_sem, 4 * number + part, seq=toggled(q, bit),
        )

    def share_start(number, part):
        _, _, length, _, give, place = plans[part][number]
        weight_out[place : place + length, lanes_of(part)] = weight_grad[
            rows_at(give, length), lanes_of(part)
        ].astype(BF16)
        share_copy(number, part).start()

    def share_finish(number, part):
        _, halves, length, keep, _, place = plans[part][number]
        with jax.named_scope("share_wait"):
            share_copy(number, part).wait()
        found = weight_in[place : place + length, lanes_of(part)].astype(F32)
        if halves:
            kept = weight_grad[rows_at(keep, length), lanes_of(part)]
        else:
            kept = weight_out[place : place + length, lanes_of(part)].astype(F32)
        weight_grad[rows_at(keep, length), lanes_of(part)] = kept + found

    def spread_copy(number, part, arrival=False):
        bit, _, length, keep, give, _ = plans[part][number]
        place = weight_all.at[rows_at(give if arrival else keep, length), lanes_of(part)]
        return remote(
            place, place, share_sem, 4 * (levels + number) + part, seq=toggled(q, bit)
        )

    def weight_event(stage, part):
        if stage < levels:
            share_finish(stage - 1, part)
            share_start(stage, part)
        elif stage == levels:
            share_finish(stage - 1, part)
            _, _, length, keep, _, _ = plans[part][-1]
            rows = rows_at(keep, length)
            weight_all[rows, lanes_of(part)] = weight_grad[rows, lanes_of(part)].astype(BF16)
            spread_copy(halvings[-1], part).start()
        else:
            number = halvings[levels - stage]
            with jax.named_scope("spread_wait"):
                spread_copy(number, part, arrival=True).wait_recv()
            if number > 0:
                spread_copy(number - 1, part).start()

    events = [(stage, part) for stage in range(1, levels + len(halvings) + 1) for part in order]
    distance = groups_along - 1 - group
    far = distance >= 2
    ready_at = jnp.where(distance == 1, messages // 2, messages - 1)

    def weights_ready():
        for slot, peer in enumerate(peers):
            with jax.named_scope("column_wait"):
                column_arrival(slot, peer).wait_recv()
        with jax.named_scope("weight_dot"):
            weight_phase(columns, cotangents, weight_grad)
        for part in order:
            share_start(0, part)

    def back_before(number):
        pl.when((number == 0) & far)(weights_ready)

    def back_step(number):
        chain_step(
            number, back_states, back_other, end_grad, back_sems,
            jnp.logical_not(odd), ends, begins, q - 2,
        )
        pl.when((number == ready_at) & jnp.logical_not(far))(weights_ready)
        for place, event in zip(CHAIN_HOOKS, events):
            pl.when((number == place) & far)(functools.partial(weight_event, *event))

    with jax.named_scope("inside_grad"):
        inside_grad_phase(
            act, cum_wide, dt_wide, cum_rows, scores, inside, scanned_grad, entering,
            scaled_grad, score_grad, query_grad, row_sums, back_before, back_step,
        )
    near = jnp.logical_not(far)

    def end_before(number):
        return_copy(back_other, end_grad, back_sems[2], number, arrival=True).wait_recv()

    def end_hook(index):
        for number in range(parts):
            pl.when((index == NEAR_HOOKS[number]) & near)(
                functools.partial(weight_event, *events[number])
            )
            pl.when((index == FAR_HOOKS[number]) & far)(
                functools.partial(weight_event, *events[number + parts])
            )

    with jax.named_scope("end"):
        end_phase(
            act, slope, cum_wide, dt_wide, cum_cols, dt_cols, decay_wide, skip_wide, scanned_grad,
            scaled_grad, score_grad, query_grad, row_sums, entering, end_grad, key_grad, skip_sum,
            step, step_bias, decay_log, raw, halo, taps, window, filtered_grad,
            step_grad, filter_sums, head_sums, end_before, end_hook,
        )
    left = events[2 * parts :]
    heads_out[...] = filtered_grad[0:8, :]
    back_copy = remote(heads_out, following, halo_sem, 1, seq=q - 1)
    pl.when(jnp.logical_not(first))(back_copy.start)

    @pl.when(last)
    def _():
        following[...] = jnp.zeros_like(following)

    small[...] = filter_sums[...]
    small[count + 1 : count + 2, 0:inner] = norm_grad[0:1, :]
    for row in range(3):
        small[count + 2 : count + 3, row * LANES : (row + 1) * LANES] = head_sums[row : row + 1, :]

    steps = [("dp", bit) for bit in (1, 2)] + [("seq", bit) for bit in bits]

    def small_copy(number):
        axis, bit = steps[number]
        target = {"seq": toggled(q, bit)} if axis == "seq" else {"dp": toggled(d, bit)}
        return remote(small_in.at[2 * number], small_in.at[2 * number + 1], small_sem, number, **target)

    def small_start(number):
        small_in[2 * number] = small[...]
        small_copy(number).start()

    def small_step(number):
        with jax.named_scope("small_wait"):
            small_copy(number).wait()
        small[...] += small_in[2 * number + 1]
        if number + 1 < len(steps):
            small_start(number + 1)

    small_start(0)

    @pl.when(near)
    def _():
        for event in events[parts : 2 * parts]:
            weight_event(*event)

    for event in left[:parts]:
        weight_event(*event)
    left = left[parts:]
    small_step(0)
    pl.when(jnp.logical_not(last))(back_copy.wait_recv)
    with jax.named_scope("filter_grad"):
        filter_grad_phase(filtered_grad, following, taps, window, input_grad)
    small_step(1)
    number = 2
    while left or number < len(steps):
        for event in left[:parts]:
            weight_event(*event)
        left = left[parts:]
        for _ in range(2 if len(left) == parts else 1):
            if number < len(steps):
                small_step(number)
                number += 1

    store_weight = pltpu.make_async_copy(weight_all, weight_result, local_sem.at[1])
    store_weight.start()
    filter_out[...] = small[0 : count + 1, :]
    for index in range(inner // LANES):
        norm_out[index : index + 1, :] = small[
            count + 1 : count + 2, index * LANES : (index + 1) * LANES
        ]
    for row in range(3):
        head_out[row : row + 1, :] = small[
            count + 2 : count + 3, row * LANES : row * LANES + step.shape[0]
        ]
    for number in halvings:
        for part in range(parts):
            spread_copy(number, part).wait_send()
    gather(d, 0, across).wait_send()
    gather(d, 1, beside).wait_send()
    gather(across, 2, beside).wait_send()
    for slot in (1, 2, 3):
        partial_copy(slot).wait_send()
    for slot, peer in enumerate(peers):
        column_copy(slot, peer).wait_send()
    pl.when(jnp.logical_not(last))(halo_copy.wait_send)
    pl.when(jnp.logical_not(first))(back_copy.wait_send)

    def drain(index, carry):
        chain_end(index, states, states_other, entering, ahead_sems, ends, q + 2)
        chain_end(index, back_states, back_other, end_grad, back_sems, begins, q - 2)
        return carry

    with jax.named_scope("drain"):
        lax.fori_loop(0, messages, drain, 0)
    store_gate.wait()
    store_weight.wait()


def body(
    conv_input,
    gate_input,
    step_input,
    filter_taps,
    filter_bias,
    step_bias,
    decay_log,
    skip_gain,
    norm_weight,
    output_weight,
    output_grad,
):
    raw, gate, step, cotangent = conv_input[0], gate_input[0], step_input[0], output_grad[0]
    tokens, channels = raw.shape
    inner = gate.shape[1]
    heads = step.shape[0]
    own_rows, width = output_weight.shape
    count = filter_taps.shape[0]
    spans, groups = lax.axis_size("seq"), lax.axis_size("dp")
    half = tokens // 2
    chunks = inner // LANES
    messages = chunks // 2
    assert groups == 4 and tokens % 256 == 0 and inner % (2 * LANES) == 0
    levels = spans.bit_length() - 1
    shared, size = 0, own_rows
    for _ in range(levels):
        size = size // 2 if size // 2 % 16 == 0 else size
        shared += size
    wide = pltpu.VMEM((tokens, inner), F32)
    full = pltpu.VMEM((tokens, channels), F32)
    columns = pltpu.VMEM((tokens, LANES), F32)
    row8 = pltpu.VMEM((8, inner), F32)
    stored = pltpu.VMEM((chunks, LANES, LANES), F32)
    turned = pltpu.VMEM((2, LANES, tokens), BF16)
    squares = pltpu.VMEM((3, half, half), F32)
    edge = pltpu.VMEM((8, channels), F32)
    sems = pltpu.SemaphoreType.DMA
    scratch = [
        pltpu.VMEM((tokens, inner), BF16), pltpu.VMEM((tokens, inner), BF16),
        pltpu.VMEM((own_rows, width), F32), edge, row8,
        pltpu.VMEM((16, channels), BF16),
        pltpu.VMEM((own_rows, width), BF16),
        pltpu.VMEM((groups, tokens, width), BF16),
        full, full, wide, wide, row8, row8,
        pltpu.VMEM((heads, 1, tokens), F32), columns, columns, turned, turned,
        pltpu.VMEM((2, tokens + 8, LANES), F32), squares,
        stored, stored, stored, wide, wide, columns,
        pltpu.VMEM((groups, tokens, own_rows), BF16),
        pltpu.VMEM((groups, tokens, own_rows), BF16),
        pltpu.VMEM((groups, tokens, own_rows), F32),
        pltpu.VMEM((groups, tokens, own_rows), BF16),
        pltpu.VMEM((tokens, own_rows), F32),
        pltpu.VMEM((2, tokens, own_rows), BF16),
        wide, wide, row8, row8,
        stored, stored, stored, squares, columns, columns, columns,
        edge, pltpu.VMEM((8, LANES), F32), edge, edge,
        pltpu.VMEM((shared, width), BF16),
        pltpu.VMEM((shared, width), BF16),
        pltpu.VMEM((own_rows, width), BF16),
        pltpu.VMEM((2 * (levels + 2), 8, channels), F32),
        sems((3,)), sems((2, 2)), sems((2, 1)), sems((2, 3)), sems((2, 3)), sems((2, 3)),
        sems((2, messages)), sems((2, messages)), sems((2, 2, messages)), sems((2, 2, messages)),
        sems((2, 8 * levels)), sems((2, levels + 2)),
    ]
    outs = [
        ((tokens, channels), BF16), ((tokens, inner), BF16), ((heads, tokens), F32),
        ((own_rows, width), BF16), ((count + 1, channels), F32), ((chunks, LANES), F32),
        ((3, heads), F32),
    ]
    args = (
        raw, step, filter_taps, filter_bias.reshape(channels // LANES, LANES),
        step_bias[None], decay_log[None], skip_gain[None],
        norm_weight.reshape(chunks, LANES), output_weight, cotangent, gate,
    )
    vmem = pl.BlockSpec(memory_space=pltpu.VMEM)
    anywhere = pl.BlockSpec(memory_space=pl.ANY)
    results = pl.pallas_call(
        functools.partial(layer_kernel, spans, groups),
        out_shape=[jax.ShapeDtypeStruct(shape, kind) for shape, kind in outs],
        in_specs=[vmem] * (len(args) - 3) + [anywhere] * 3,
        out_specs=[vmem, anywhere, vmem, anywhere, vmem, vmem, vmem],
        scratch_shapes=scratch,
        compiler_params=pltpu.CompilerParams(
            vmem_limit_bytes=67043328, has_side_effects=True, collective_id=0
        ),
    )(*args)
    kinds = [outs[number] for number in range(len(outs))]
    kinds[3] = ((own_rows, width), F32)
    input_grad, gate_grad, step_grad, weight_grad, filter_grads, norm_grad, head_grads = pl.pallas_call(
        finish_kernel,
        out_shape=[jax.ShapeDtypeStruct(shape, kind) for shape, kind in kinds],
        in_specs=[anywhere] * len(outs),
        out_specs=[anywhere] * len(outs),
        scratch_shapes=[pltpu.VMEM(*out) for out in outs]
        + [pltpu.VMEM(*kinds[3]), sems((len(outs),)), sems((len(outs),))],
        compiler_params=pltpu.CompilerParams(vmem_limit_bytes=67043328),
    )(*results)
    return (
        input_grad[None], gate_grad[None], step_grad[None], weight_grad,
        filter_grads, norm_grad.reshape(inner), head_grads,
    )


def finish_kernel(*refs):
    count = (len(refs) - 3) // 3
    sources, targets, held = refs[:count], refs[count : 2 * count], list(refs[2 * count : 3 * count])
    widened, load_sem, store_sem = refs[3 * count :]
    loads = [
        pltpu.make_async_copy(source, buffer, load_sem.at[number])
        for number, (source, buffer) in enumerate(zip(sources, held))
    ]
    order = [3] + [number for number in range(count) if number != 3]
    for number in order:
        loads[number].start()
    stores = []
    for number in order:
        loads[number].wait()
        buffer = held[number]
        if number == 3:
            widened[...] = buffer[...].astype(F32)
            buffer = widened
        store = pltpu.make_async_copy(buffer, targets[number], store_sem.at[number])
        store.start()
        stores.append(store)
    for store in stores:
        store.wait()


def solution(mesh):
    return jax.shard_map(
        body,
        mesh=mesh,
        in_specs=(
            P("dp", "seq", None),
            P("dp", "seq", None),
            P("dp", None, "seq"),
            P(),
            P(),
            P(),
            P(),
            P(),
            P(),
            P("dp", None),
            P("dp", "seq", None),
        ),
        out_specs=(
            P("dp", "seq", None),
            P("dp", "seq", None),
            P("dp", None, "seq"),
            P("dp", None),
            P(),
            P(),
            P(),
        ),
        check_vma=False,
    )
```

```python
import functools

import jax
import jax.numpy as jnp
from jax import lax
from jax.experimental import pallas as pl
from jax.experimental.pallas import tpu as pltpu
from jax.sharding import PartitionSpec as P

F32 = jnp.float32
BF16 = jnp.bfloat16
EPSILON = 1e-05
LOG2E = 1.4426950408889634
LANES = 128
HEAD_DIM = 64
MESH = pl.DeviceIdType.MESH
CHAIN_HOOKS = (6, 6, 9, 9)
FAR_HOOKS = (4, 4, 8, 8)
NEAR_HOOKS = (6, 6, 9, 9)
NN = (((1,), (0,)), ((), ()))
NT = (((1,), (1,)), ((), ()))
TN = (((0,), (0,)), ((), ()))


def dot(a, b, dims=NN):
    return lax.dot_general(a, b, dims, preferred_element_type=F32)


def rounded_high(a):
    scaled = a * 65537.0
    return scaled - (scaled - a)


def split2(a):
    high = rounded_high(a)
    return high.astype(BF16), (a - high).astype(BF16)


def split3(a):
    high = rounded_high(a)
    rest = a - high
    middle = rounded_high(rest)
    return high.astype(BF16), middle.astype(BF16), (rest - middle).astype(BF16)


def dot3(a, b, dims=NN):
    return dot(a[0], b[0], dims) + (dot(a[0], b[1], dims) + dot(a[1], b[0], dims))


def chunk_of(index):
    return pl.ds(pl.multiple_of(index * LANES, LANES), LANES)


def iota(shape, dim):
    return lax.broadcasted_iota(jnp.int32, shape, dim)


def low_half(shape):
    return iota(shape, 1) < HEAD_DIM


def head_rows(index):
    shape = (LANES, LANES)
    wanted = 2 * index + jnp.where(low_half(shape), 0, 1)
    return jnp.where(iota(shape, 0) == wanted, 1.0, 0.0).astype(BF16)


def sigmoid(a):
    return 1.0 / (1.0 + jnp.exp(-a))


def transposed(rows):
    heads, tokens = rows.shape
    padded = jnp.concatenate([rows, jnp.zeros((LANES - heads, tokens), F32)], axis=0)
    return padded.T


def padded_row(row):
    short = row[...]
    return jnp.concatenate([short, jnp.zeros((1, LANES - short.shape[1]), F32)], axis=1)


def column_of(row):
    return jnp.broadcast_to(padded_row(row), (LANES, LANES)).T[: row.shape[1], 0:1]


def step_phase(step, step_bias, decay_log, cum_rows, cum_cols, dt_cols):
    shifted = step[...] + column_of(step_bias)
    sizes = jnp.maximum(shifted, 0.0) + jnp.log1p(jnp.exp(-jnp.abs(shifted)))
    rates = -jnp.exp(column_of(decay_log)) * sizes
    tokens = rates.shape[1]
    shape = (tokens, tokens)
    before = jnp.where(iota(shape, 0) <= iota(shape, 1), 1.0, 0.0).astype(BF16)
    high, middle, low = split3(rates)
    cumulative = (dot(high, before) + (dot(middle, before) + dot(low, before))) * LOG2E
    for head in range(rates.shape[0]):
        cum_rows[head] = cumulative[head : head + 1]
    cum_cols[...] = transposed(cumulative)
    dt_cols[...] = transposed(sizes)


def expand_phase(cum_cols, dt_cols, skip_gain, cum_wide, dt_wide, decay_wide, skip_wide):
    tokens, inner = cum_wide.shape
    cum_parts = split3(cum_cols[...])
    dt_parts = split3(dt_cols[...])
    skip_parts = split3(jnp.broadcast_to(padded_row(skip_gain), (8, LANES)))

    def each(index, carry):
        here = chunk_of(index)
        rows = head_rows(index)
        wide = dot(cum_parts[0], rows) + (dot(cum_parts[1], rows) + dot(cum_parts[2], rows))
        cum_wide[:, here] = wide
        skip_wide[:, here] = dot(skip_parts[0], rows) + (
            dot(skip_parts[1], rows) + dot(skip_parts[2], rows)
        )
        dt_wide[:, here] = dot(dt_parts[0], rows) + (
            dot(dt_parts[1], rows) + dot(dt_parts[2], rows)
        )
        decay_wide[:, here] = jnp.broadcast_to(jnp.exp2(wide[tokens - 1 : tokens]), (8, LANES))
        return carry

    lax.fori_loop(0, inner // LANES, each, 0, unroll=4)


def filter_chunk(index, slot, here, raw, halo, taps, bias, windows, act, slope):
    tokens = raw.shape[0]
    window = windows.at[slot]
    window[0:8, :] = halo[:, here].astype(F32)[8:]
    window[8 : 8 + tokens, :] = raw[:, here].astype(F32)
    count = taps.shape[0]
    filtered = bias[pl.ds(index, 1), :] + taps[0:1, here] * window[9 - count : 9 - count + tokens, :]
    for k in range(1, count):
        filtered = filtered + taps[k : k + 1, here] * window[9 - count + k : 9 - count + k + tokens, :]
    gate = sigmoid(filtered)
    result = filtered * gate
    act[:, here] = result
    slope[:, here] = gate + result * (1.0 - gate)
    return result


def in_pairs(total, before, after, each, carry):
    def several(number, carry):
        if before is not None:
            before(number)
        for j in range(2):
            carry = each(2 * number + j, carry, j)
        if after is not None:
            after(number)
        return carry

    return lax.fori_loop(0, total // 2, several, carry)


def state_phase(
    raw, halo, taps, bias, window, act, slope, cum_wide, dt_wide, key_t, query_t, states, after
):
    tokens, inner = cum_wide.shape
    first = inner // LANES
    key = filter_chunk(first, 0, pl.ds(inner, LANES), raw, halo, taps, bias, window, act, slope)
    query = filter_chunk(first + 1, 1, pl.ds(inner + LANES, LANES), raw, halo, taps, bias, window, act, slope)
    high, low = split2(key.T)
    key_t[0], key_t[1] = high, low
    high, low = split2(query.T)
    query_t[0], query_t[1] = high, low

    def each(index, carry, slot):
        here = chunk_of(index)
        values = filter_chunk(index, slot, here, raw, halo, taps, bias, window, act, slope)
        cum = cum_wide[:, here]
        moved = values * dt_wide[:, here] * jnp.exp2(cum[tokens - 1 : tokens] - cum)
        states[index] = dot3((key_t[0], key_t[1]), split2(moved))
        return carry

    in_pairs(first, None, after, each, 0)


def score_blocks(act, inner, scores):
    half = act.shape[0] // 2
    key = split2(act[:, inner : inner + LANES])
    query = split2(act[:, inner + LANES : inner + 2 * LANES])
    shape = (half, half)
    causal = iota(shape, 0) >= iota(shape, 1)
    for slot, (rows, columns) in enumerate(((0, 0), (1, 1), (1, 0))):
        left = tuple(part[rows * half : (rows + 1) * half] for part in query)
        right = tuple(part[columns * half : (columns + 1) * half] for part in key)
        block = dot3(left, right, NT)
        if rows == columns:
            block = jnp.where(causal, block, 0.0)
        scores[slot] = block


def decay_blocks(index, cum, cum_rows, half, block):
    rows = slice(block * half, (block + 1) * half)
    found = []
    for j in range(2):
        column = jnp.broadcast_to(cum[rows, j * HEAD_DIM : j * HEAD_DIM + 1], (half, half))
        row = cum_rows[2 * index + j][:, rows]
        found.append(jnp.exp2(jnp.minimum(column - row, 0.0)))
    return jnp.concatenate(found, axis=1)


def stacked(block):
    low = low_half(block.shape)
    zero = jnp.zeros_like(block)
    return jnp.concatenate([jnp.where(low, block, zero), jnp.where(low, zero, block)], axis=0)


def inside_phase(act, cum_wide, dt_wide, cum_rows, scores, inside, before, after):
    tokens, inner = cum_wide.shape
    half = tokens // 2

    def each(index, carry, slot):
        here = chunk_of(index)
        scaled = act[:, here] * dt_wide[:, here]
        cum = cum_wide[:, here]
        for block in range(2):
            rows = slice(block * half, (block + 1) * half)
            weights = decay_blocks(index, cum, cum_rows, half, block)
            score = scores[block]
            weights = jnp.concatenate([score, score], axis=1) * weights
            right = stacked(scaled[rows])
            result = dot3(split2(weights), split2(right))
            if block == 1:
                middle = cum[half - 1 : half]
                moved = scaled[:half] * jnp.exp2(middle - cum[:half])
                result = result + jnp.exp2(cum[half:] - middle) * dot3(
                    split2(scores[2]), split2(moved)
                )
            inside[rows, here] = result
        return carry

    in_pairs(inner // LANES, before, after, each, 0)


def norm_phase(act, cum_wide, inside, entering, skip_wide, gate, norm_weight, gated, scale, low):
    tokens, inner = cum_wide.shape
    query = split2(act[:, inner + LANES : inner + 2 * LANES])

    def each(index, total):
        here = chunk_of(index)
        crossed = jnp.exp2(cum_wide[:, here]) * dot3(query, split2(entering[index]))
        scanned = inside[:, here] + crossed
        inside[:, here] = scanned
        scanned = scanned + skip_wide[0:1, here] * act[:, here]
        branch = gate[:, here].astype(F32)
        result = scanned * (branch * sigmoid(branch))
        gated[:, here] = result
        return total + result * result

    total = lax.fori_loop(0, inner // LANES, each, jnp.zeros((tokens, LANES), F32), unroll=2)
    mean = jnp.sum(total, axis=1, keepdims=True) / inner
    inverse = lax.rsqrt(mean + EPSILON)
    scale[...] = jnp.broadcast_to(inverse, scale.shape)

    per = low.shape[2] // LANES

    def rounded(index, carry):
        here = chunk_of(index)
        place = pl.ds(pl.multiple_of(index % per * LANES, LANES), LANES)
        result = gated[:, here] * scale[...] * norm_weight[pl.ds(index, 1), :]
        low[index // per, :, place] = result.astype(BF16)
        return carry

    lax.fori_loop(0, inner // LANES, rounded, 0)


def gate_phase(
    act, cum_wide, inside, skip_wide, gate, norm_weight, gated, scale, query_t,
    chip, normed_sent, normed_grad, scanned_grad, gate_grad, norm_grad, skip_sum, entering_grad,
    after,
):
    tokens, inner = cum_wide.shape

    per = normed_grad.shape[2] // LANES

    def normed_at(index):
        return normed_grad[index // per, :, chunk_of(index % per)]

    def first(index, total):
        here = chunk_of(index)
        slot, place = index // per, chunk_of(index % per)
        sent = normed_sent[slot, :, place].astype(F32)
        found = jnp.where(slot // 2 == chip, normed_grad[slot, :, place], sent)
        normed_grad[slot, :, place] = found
        return total + found * norm_weight[pl.ds(index, 1), :] * gated[:, here]

    total = lax.fori_loop(0, inner // LANES, first, jnp.zeros((tokens, LANES), F32), unroll=2)
    inverse = scale[...]
    pull = jnp.sum(total, axis=1, keepdims=True) / inner * inverse * inverse * inverse

    def second(index, carry, slot):
        here = chunk_of(index)
        found = normed_at(index)
        product = gated[:, here]
        norm_grad[:, here] = jnp.broadcast_to(
            jnp.sum(found * product * inverse, axis=0, keepdims=True), (8, LANES)
        )
        down = inverse * (found * norm_weight[pl.ds(index, 1), :]) - product * pull
        branch = gate[:, here].astype(F32)
        opened = sigmoid(branch)
        passed = branch * opened
        values = act[:, here]
        scanned = inside[:, here] + skip_wide[0:1, here] * values
        gate_grad[:, here] = (down * scanned * (opened + passed * (1.0 - opened))).astype(BF16)
        back = down * passed
        scanned_grad[:, here] = back
        skip_sum[:, here] = jnp.broadcast_to(
            jnp.sum(back * values, axis=0, keepdims=True), (8, LANES)
        )
        moved = back * jnp.exp2(cum_wide[:, here])
        entering_grad[index] = dot3((query_t[0], query_t[1]), split2(moved))
        return carry

    in_pairs(inner // LANES, None, after, second, 0)


def inside_grad_phase(
    act, cum_wide, dt_wide, cum_rows, scores, inside, scanned_grad, entering,
    scaled_grad, score_grad, query_grad, row_sums, before, after,
):
    tokens, inner = cum_wide.shape
    half = tokens // 2
    score_grad[...] = jnp.zeros_like(score_grad)
    query_grad[...] = jnp.zeros_like(query_grad)
    row_sums[...] = jnp.zeros_like(row_sums)

    def each(index, carry, slot):
        here = chunk_of(index)
        scaled = act[:, here] * dt_wide[:, here]
        cum = cum_wide[:, here]
        back = scanned_grad[:, here]
        middle = cum[half - 1 : half]
        for block in range(2):
            rows = slice(block * half, (block + 1) * half)
            decay = decay_blocks(index, cum, cum_rows, half, block)
            score = scores[block]
            weights = split2(jnp.concatenate([score, score], axis=1) * decay)
            down = split2(back[rows])
            products = dot3(down, split2(stacked(scaled[rows])), NT) * decay
            score_grad[block] += products[:, :half] + products[:, half:]
            found = dot3(weights, down, TN)
            found = jnp.where(low_half((half, LANES)), found[:half], found[half:])
            if block == 0:
                pulled = split2(back[half:] * jnp.exp2(cum[half:] - middle))
                factor = jnp.exp2(middle - cum[:half])
                score_grad[2] += dot3(pulled, split2(scaled[:half] * factor), NT)
                found = found + factor * dot3(split2(scores[2]), pulled, TN)
            scaled_grad[rows, here] = found
        query_grad[...] += dot3(split2(back * jnp.exp2(cum)), split2(entering[index]), NT)
        rows = head_rows(index)
        high, low = split2(back * inside[:, here])
        row_sums[...] += dot(high, rows, NT) + dot(low, rows, NT)
        return carry

    in_pairs(inner // LANES, before, after, each, 0)


def end_phase(
    act, slope, cum_wide, dt_wide, cum_cols, dt_cols, decay_wide, skip_wide, scanned_grad,
    scaled_grad, score_grad, query_grad, row_sums, entering, end_grad, key_grad, skip_sum,
    step, step_bias, decay_log, raw, halo, taps, windows, filtered_grad,
    step_grad, filter_sums, head_sums, before_pair, after_pair,
):
    tokens, inner = cum_wide.shape
    half = tokens // 2
    key = split2(act[:, inner : inner + LANES])
    query = split2(act[:, inner + LANES : inner + 2 * LANES])
    count = taps.shape[0]

    def finish(slot, here, found):
        pulled = found * slope[:, here]
        filtered_grad[:, here] = pulled
        window = windows.at[slot]
        window[0:8, :] = halo[:, here].astype(F32)[8:]
        window[8 : 8 + tokens, :] = raw[:, here].astype(F32)
        sums = [
            jnp.sum(pulled * window[9 - count + k : 9 - count + k + tokens, :], axis=0, keepdims=True)
            for k in range(count)
        ]
        sums.append(jnp.sum(pulled, axis=0, keepdims=True))
        sums.append(jnp.zeros((8 - len(sums), LANES), F32))
        filter_sums[:, here] = jnp.concatenate(sums, axis=0)

    key_grad[...] = jnp.zeros_like(key_grad)
    zeros = (jnp.zeros((tokens, LANES), F32), jnp.zeros((8, LANES), F32), jnp.zeros((8, LANES), F32))

    def each(index, sums, slot):
        value_sums, last_sums, skip_sums = sums
        here = chunk_of(index)
        values = act[:, here]
        sizes = dt_wide[:, here]
        cum = cum_wide[:, here]
        to_end = jnp.exp2(cum[tokens - 1 : tokens] - cum)
        after = end_grad[index]
        parts = split2(after)
        moved = values * sizes * to_end
        moved_grad = dot3(key, parts)
        key_grad[...] += dot3(split2(moved), parts, NT)
        last = jnp.sum(moved * moved_grad, axis=0, keepdims=True) + decay_wide[0:1, here] * jnp.sum(
            after * entering[index], axis=0, keepdims=True
        )
        scaled = scaled_grad[:, here] + to_end * moved_grad
        rows = head_rows(index)
        high, low = split2(scaled * values)
        value_sums = value_sums + (dot(high, rows, NT) + dot(low, rows, NT))
        parts = split3(jnp.broadcast_to(last, (8, LANES)))
        last_sums = last_sums + (dot(parts[0], rows, NT) + (dot(parts[1], rows, NT) + dot(parts[2], rows, NT)))
        parts = split3(skip_sum[:, here])
        skip_sums = skip_sums + (dot(parts[0], rows, NT) + (dot(parts[1], rows, NT) + dot(parts[2], rows, NT)))
        finish(slot, here, scaled * sizes + skip_wide[0:1, here] * scanned_grad[:, here])
        return value_sums, last_sums, skip_sums

    value_sums, last_sums, skip_sums = in_pairs(inner // LANES, before_pair, after_pair, each, zeros)

    shape = (half, half)
    causal = iota(shape, 0) >= iota(shape, 1)
    blocks = [split2(jnp.where(causal, score_grad[slot], 0.0)) for slot in range(2)]
    blocks.append(split2(score_grad[2]))
    first = lambda parts: tuple(part[:half] for part in parts)
    second = lambda parts: tuple(part[half:] for part in parts)
    upper = dot3(blocks[0], first(key))
    lower = dot3(blocks[1], second(key)) + dot3(blocks[2], first(key))
    finish(1, pl.ds(inner + LANES, LANES), query_grad[...] + jnp.concatenate([upper, lower], axis=0))
    upper = dot3(blocks[0], first(query), TN) + dot3(blocks[2], second(query), TN)
    lower = dot3(blocks[1], second(query), TN)
    finish(0, pl.ds(inner, LANES), key_grad[...] + jnp.concatenate([upper, lower], axis=0))

    sizes = dt_cols[...]
    cum_grad = row_sums[...] - sizes * value_sums
    at_end = iota((tokens, LANES), 0) == tokens - 1
    cum_grad = cum_grad + jnp.where(at_end, jnp.broadcast_to(last_sums[0:1], (tokens, LANES)), 0.0)
    shape = (tokens, tokens)
    after = jnp.where(iota(shape, 0) <= iota(shape, 1), 1.0, 0.0).astype(BF16)
    parts = split3(cum_grad)
    rate_grad = dot(after, parts[0]) + (dot(after, parts[1]) + dot(after, parts[2]))
    rate = -jnp.exp(padded_row(decay_log))
    heads = step.shape[0]
    shifted = transposed(step[...] + column_of(step_bias))
    pulled = (value_sums + rate_grad * rate) * sigmoid(shifted)
    pulled = jnp.where(iota((tokens, LANES), 1) < heads, pulled, 0.0)
    step_grad[...] = pulled.T[:heads]
    head_sums[...] = jnp.concatenate(
        [
            jnp.sum(pulled, axis=0, keepdims=True),
            jnp.sum(rate_grad * rate * sizes, axis=0, keepdims=True),
            skip_sums[0:1],
            jnp.zeros((5, LANES), F32),
        ],
        axis=0,
    )


def filter_grad_phase(filtered_grad, following, taps, windows, input_grad):
    tokens, channels = filtered_grad.shape
    count = taps.shape[0]

    def each(index, carry, slot):
        here = chunk_of(index)
        window = windows.at[slot]
        window[0:tokens, :] = filtered_grad[:, here]
        window[tokens : tokens + 8, :] = following[:, here]
        total = taps[count - 1 : count, here] * window[0:tokens, :]
        for k in range(count - 1):
            offset = count - 1 - k
            total = total + taps[k : k + 1, here] * window[offset : offset + tokens, :]
        input_grad[:, here] = total.astype(BF16)
        return carry

    in_pairs(channels // LANES, None, None, each, 0)


def toggled(index, bit):
    return index + bit - 2 * bit * (index // bit % 2)


def weight_phase(columns, cotangents, total):
    peers, tokens, rows = columns.shape

    def each(index, carry):
        here = chunk_of(index)
        found = dot(columns[0, :, here], cotangents[0], TN)
        for peer in range(1, peers):
            found = found + dot(columns[peer, :, here], cotangents[peer], TN)
        total[pl.ds(pl.multiple_of(index * LANES, LANES), LANES), :] = found
        return carry

    lax.fori_loop(0, rows // LANES, each, 0)


def layer_kernel(
    spans, groups,
    raw, step, taps, bias, step_bias, decay_log, skip_gain, norm_weight,
    weight, cotangent, gate_in,
    input_grad, gate_out, step_grad, weight_result, filter_out, norm_out, head_out,
    gate, gate_grad, weight_grad, small, skip_wide, halo, weights, cotangents, act, slope, cum_wide, dt_wide, decay_wide, other_decay,
    cum_rows, cum_cols, dt_cols, key_t, query_t, window, scores,
    states, states_other, entering, inside, gated, scale, low, columns,
    normed_grad, normed_sent, partial_beside, partials, scaled_grad, scanned_grad, norm_grad, skip_sum,
    back_states, back_other, end_grad, score_grad, query_grad, row_sums, key_grad,
    filter_sums, head_sums, following, heads_out,
    weight_out, weight_in, weight_all, small_in,
    local_sem, halo_sem, decay_sem, gather_sem, partial_sem, column_sem, ahead_sem, back_sem, next_sem, return_sem,
    share_sem, small_sem,
):
    q, d = lax.axis_index("seq"), lax.axis_index("dp")
    tokens, channels = raw.shape
    inner = gate_in.shape[1]
    own_rows = weight.shape[0]
    count = taps.shape[0]
    filtered_grad = act

    def remote(source, target, sems, slot, seq=None, dp=None):
        return pltpu.make_async_remote_copy(
            src_ref=source,
            dst_ref=target,
            send_sem=sems.at[0, slot],
            recv_sem=sems.at[1, slot],
            device_id=(q if seq is None else seq, d if dp is None else dp),
            device_id_type=MESH,
        )

    first, last = q == 0, q == spans - 1
    partner = toggled(q, 1)
    odd = q % 2 == 1
    group, groups_along = q // 2, spans // 2

    load_weight = pltpu.make_async_copy(weight, weights, local_sem.at[0])
    load_cotangent = pltpu.make_async_copy(cotangent, cotangents.at[d], local_sem.at[1])
    load_gate = pltpu.make_async_copy(gate_in, gate, local_sem.at[2])
    load_cotangent.start()
    load_weight.start()
    load_gate.start()

    across, beside = toggled(d, 2), toggled(d, 1)
    bits = []
    while 2 ** len(bits) < spans:
        bits.append(2 ** len(bits))
    barrier = pltpu.get_barrier_semaphore()

    def greet(seq, dp):
        pl.semaphore_signal(barrier, inc=1, device_id=(seq, dp), device_id_type=MESH)

    for other in (across, beside, toggled(across, 1)):
        greet(q, other)
    for bit in bits:
        greet(toggled(q, bit), d)
    expected = 3 + len(bits)
    for distance in (1, 2):
        below, above = q >= distance, q < spans - distance
        pl.when(below)(lambda distance=distance: greet(q - distance, d))
        pl.when(above)(lambda distance=distance: greet(q + distance, d))
        expected = expected + jnp.where(below, 1, 0) + jnp.where(above, 1, 0)

    with jax.named_scope("steps"):
        step_phase(step, step_bias, decay_log, cum_rows, cum_cols, dt_cols)
    with jax.named_scope("barrier"):
        pl.semaphore_wait(barrier, expected)

    with jax.named_scope("halo_start"):
        halo_copy = remote(raw.at[tokens - 16 : tokens], halo, halo_sem, 0, seq=q + 1)
    pl.when(jnp.logical_not(last))(halo_copy.start)

    @pl.when(first)
    def _():
        halo[...] = jnp.zeros_like(halo)

    diagonal = toggled(across, 1)

    def gather(owner, slot, target):
        place = cotangents.at[owner]
        return remote(place, place, gather_sem, slot, dp=target)

    load_cotangent.wait()
    gather(d, 0, across).start()
    gather(d, 1, beside).start()

    with jax.named_scope("expand"):
        expand_phase(cum_cols, dt_cols, skip_gain, cum_wide, dt_wide, decay_wide, skip_wide)
    decay_copy = remote(decay_wide, other_decay, decay_sem, 0, seq=partner)
    decay_copy.start()
    pl.when(jnp.logical_not(first))(halo_copy.wait_recv)

    side = q % 2

    def pair_copy(source, target, sems, number, arrival=False):
        at = 2 * number + (side if arrival else 1 - side)
        return remote(source.at[at], target.at[at], sems, number, seq=partner)

    with jax.named_scope("states"):
        state_phase(
            raw, halo, taps, bias, window, act, slope, cum_wide, dt_wide, key_t, query_t, states,
            lambda number: pair_copy(states, states_other, ahead_sem, number).start(),
        )
    with jax.named_scope("decay"):
        decay_copy.wait()
    score_blocks(act, inner, scores)

    def chain_copy(own, arrived, sems, number, towards):
        at = 2 * number + side
        return remote(own.at[at], arrived.at[at], sems, number, seq=towards)

    def return_copy(other, arrived, sems, number, arrival=False):
        at = 2 * number + (1 - side if arrival else side)
        return remote(other.at[at], arrived.at[at], sems, number, seq=partner)

    def chain_step(number, own, other, arrived, sems, late, begins, ends, towards):
        pair_sem, chain_sem, return_sem = sems
        chain = chain_copy(own, arrived, chain_sem, number, towards)
        with jax.named_scope("pair_wait"):
            pair_copy(own, other, pair_sem, number, arrival=True).wait_recv()
        with jax.named_scope("chain_wait"):
            pl.when(jnp.logical_not(begins))(chain.wait_recv)
        at = 2 * number + side
        here = chunk_of(at)
        mine, theirs = own[at], other[at]
        mine_decay, their_decay = decay_wide[0:1, here], other_decay[0:1, here]
        running = jnp.where(begins, 0.0, arrived[at])
        both = jnp.where(late, mine_decay * theirs + mine, their_decay * mine + theirs)
        own[at] = mine_decay * their_decay * running + both
        pl.when(jnp.logical_not(ends))(chain.start)
        arrived[at] = jnp.where(late, theirs + their_decay * running, running)
        other[at] = jnp.where(late, running, mine + mine_decay * running)
        return_copy(other, arrived, return_sem, number).start()

    def chain_end(number, own, other, arrived, sems, ends, towards):
        pair_sem, chain_sem, return_sem = sems
        pair_copy(own, other, pair_sem, number).wait_send()
        chain = chain_copy(own, arrived, chain_sem, number, towards)
        pl.when(jnp.logical_not(ends))(chain.wait_send)
        return_copy(other, arrived, return_sem, number).wait_send()

    messages = states.shape[0] // 2
    ahead_sems = (ahead_sem, next_sem.at[0], return_sem.at[0])
    back_sems = (back_sem, next_sem.at[1], return_sem.at[1])
    begins, ends = group == 0, group == groups_along - 1

    per_slot = own_rows // LANES
    owners = (d, beside, across, diagonal)
    load_weight.wait()

    def partial_copy(slot, arrival=False):
        owner = owners[slot]
        lands = owner if arrival else d
        if slot == 1:
            return remote(partial_beside, normed_grad.at[lands], partial_sem, 0, dp=owner)
        return remote(partials.at[slot - 2], normed_sent.at[lands], partial_sem, slot - 1, dp=owner)

    def partial_chunk(number):
        slot = number // per_slot
        owner = owners[3]
        for other in (2, 1, 0):
            owner = jnp.where(slot == other, owners[other], owner)
        index = number % per_slot
        rows = weights[pl.ds(pl.multiple_of(index * LANES, LANES), LANES), :]
        found = dot(cotangents[owner], rows, NT)

        @pl.when(slot == 0)
        def _():
            normed_grad[d, :, chunk_of(index)] = found

        @pl.when(slot == 1)
        def _():
            partial_beside[:, chunk_of(index)] = found

        @pl.when(slot > 1)
        def _():
            partials[slot - 2, :, chunk_of(index)] = found.astype(BF16)

        for slot in (1, 2, 3):
            pl.when(number == (slot + 1) * per_slot - 1)(partial_copy(slot).start)

    early = group < 2

    def across_arrives():
        gather(across, 0, across).wait_recv()
        gather(across, 2, beside).start()

    def partial_slots(first, last):
        def each(at, carry):
            partial_chunk(at)
            return carry

        lax.fori_loop(first * per_slot, last * per_slot, each, 0)

    def ahead_before(number):
        @pl.when((number == 0) & jnp.logical_not(early))
        def _():
            gather(beside, 1, beside).wait_recv()
            partial_slots(0, 2)
            across_arrives()
            partial_slots(2, 3)
            gather(diagonal, 2, beside).wait_recv()
            partial_slots(3, 4)

    def ahead_step(number):
        chain_step(
            number, states, states_other, entering, ahead_sems, odd, begins, ends, q + 2
        )

        pl.when(early & (number == per_slot))(across_arrives)
        pl.when(early & (number == per_slot + per_slot // 2))(gather(diagonal, 2, beside).wait_recv)

        @pl.when(early & (number >= per_slot))
        def _():
            for j in range(2):
                partial_chunk(2 * number + j)

    with jax.named_scope("inside"):
        inside_phase(
            act, cum_wide, dt_wide, cum_rows, scores, inside, ahead_before, ahead_step,
        )

    @pl.when(early)
    def _():
        gather(beside, 1, beside).wait_recv()
        partial_slots(0, 2)

    with jax.named_scope("return_wait"):
        for number in range(messages):
            return_copy(states_other, entering, ahead_sems[2], number, arrival=True).wait_recv()
    load_gate.wait()
    with jax.named_scope("norm"):
        norm_phase(act, cum_wide, inside, entering, skip_wide, gate, norm_weight, gated, scale, low)

    def column_copy(slot, peer):
        return remote(low.at[peer], columns.at[d], column_sem, slot, dp=peer)

    def column_arrival(slot, peer):
        return remote(low.at[peer], columns.at[peer], column_sem, slot, dp=peer)

    peers = (across, diagonal, beside)
    for slot, peer in enumerate(peers):
        column_copy(slot, peer).start()
    columns[d] = low[d]
    with jax.named_scope("partial_wait"):
        for slot in (1, 2, 3):
            partial_copy(slot, arrival=True).wait_recv()

    with jax.named_scope("gate"):
        gate_phase(
            act, cum_wide, inside, skip_wide, gate, norm_weight, gated, scale, query_t,
            d // 2, normed_sent, normed_grad, scanned_grad, gate_grad, norm_grad, skip_sum,
            back_states,
            lambda number: pair_copy(back_states, back_other, back_sem, number).start(),
        )

    store_gate = pltpu.make_async_copy(gate_grad, gate_out, local_sem.at[0])
    store_gate.start()

    def plan_for(order):
        size, base, offset = own_rows, 0, 0
        plan = []
        for bit in order:
            mine = q // bit % 2
            halves = size // 2 % 16 == 0
            if halves:
                size = size // 2
                keep, give = base + mine * size, base + (1 - mine) * size
                base = keep
            else:
                keep, give = base, base
            plan.append((bit, halves, size, keep, give, offset))
            offset = offset + size
        return plan

    plans = (plan_for(bits), plan_for(bits[1:] + bits[:1])) * 2
    levels = len(bits)
    halvings = [number for number in range(levels) if plans[0][number][1]]
    tiles = cotangent.shape[1] // LANES
    parts = 4
    edges = [-(-tiles * part // parts) * LANES for part in range(parts + 1)]
    order = (1, 3, 0, 2)

    def rows_at(start, length):
        return pl.ds(pl.multiple_of(start, 16), length)

    def lanes_of(part):
        return pl.ds(edges[part], edges[part + 1] - edges[part])

    def share_copy(number, part):
        bit, _, length, _, _, place = plans[part][number]
        rows = pl.ds(place, length)
        return remote(
            weight_out.at[rows, lanes_of(part)], weight_in.at[rows, lanes_of(part)],
            share_sem, 4 * number + part, seq=toggled(q, bit),
        )

    def share_start(number, part):
        _, _, length, _, give, place = plans[part][number]
        weight_out[place : place + length, lanes_of(part)] = weight_grad[
            rows_at(give, length), lanes_of(part)
        ].astype(BF16)
        share_copy(number, part).start()

    def share_finish(number, part):
        _, halves, length, keep, _, place = plans[part][number]
        with jax.named_scope("share_wait"):
            share_copy(number, part).wait()
        found = weight_in[place : place + length, lanes_of(part)].astype(F32)
        if halves:
            kept = weight_grad[rows_at(keep, length), lanes_of(part)]
        else:
            kept = weight_out[place : place + length, lanes_of(part)].astype(F32)
        weight_grad[rows_at(keep, length), lanes_of(part)] = kept + found

    def spread_copy(number, part, arrival=False):
        bit, _, length, keep, give, _ = plans[part][number]
        place = weight_all.at[rows_at(give if arrival else keep, length), lanes_of(part)]
        return remote(
            place, place, share_sem, 4 * (levels + number) + part, seq=toggled(q, bit)
        )

    def weight_event(stage, part):
        if stage < levels:
            share_finish(stage - 1, part)
            share_start(stage, part)
        elif stage == levels:
            share_finish(stage - 1, part)
            _, _, length, keep, _, _ = plans[part][-1]
            rows = rows_at(keep, length)
            weight_all[rows, lanes_of(part)] = weight_grad[rows, lanes_of(part)].astype(BF16)
            spread_copy(halvings[-1], part).start()
        else:
            number = halvings[levels - stage]
            with jax.named_scope("spread_wait"):
                spread_copy(number, part, arrival=True).wait_recv()
            if number > 0:
                spread_copy(number - 1, part).start()

    events = [(stage, part) for stage in range(1, levels + len(halvings) + 1) for part in order]
    distance = groups_along - 1 - group
    far = distance >= 2
    ready_at = jnp.where(distance == 1, messages // 2, messages - 1)

    def weights_ready():
        for slot, peer in enumerate(peers):
            with jax.named_scope("column_wait"):
                column_arrival(slot, peer).wait_recv()
        with jax.named_scope("weight_dot"):
            weight_phase(columns, cotangents, weight_grad)
        for part in order:
            share_start(0, part)

    def back_before(number):
        pl.when((number == 0) & far)(weights_ready)

    def back_step(number):
        chain_step(
            number, back_states, back_other, end_grad, back_sems,
            jnp.logical_not(odd), ends, begins, q - 2,
        )
        pl.when((number == ready_at) & jnp.logical_not(far))(weights_ready)
        for place, event in zip(CHAIN_HOOKS, events):
            pl.when((number == place) & far)(functools.partial(weight_event, *event))

    with jax.named_scope("inside_grad"):
        inside_grad_phase(
            act, cum_wide, dt_wide, cum_rows, scores, inside, scanned_grad, entering,
            scaled_grad, score_grad, query_grad, row_sums, back_before, back_step,
        )
    near = jnp.logical_not(far)

    def end_before(number):
        return_copy(back_other, end_grad, back_sems[2], number, arrival=True).wait_recv()

    def end_hook(index):
        for number in range(parts):
            pl.when((index == NEAR_HOOKS[number]) & near)(
                functools.partial(weight_event, *events[number])
            )
            pl.when((index == FAR_HOOKS[number]) & far)(
                functools.partial(weight_event, *events[number + parts])
            )

    with jax.named_scope("end"):
        end_phase(
            act, slope, cum_wide, dt_wide, cum_cols, dt_cols, decay_wide, skip_wide, scanned_grad,
            scaled_grad, score_grad, query_grad, row_sums, entering, end_grad, key_grad, skip_sum,
            step, step_bias, decay_log, raw, halo, taps, window, filtered_grad,
            step_grad, filter_sums, head_sums, end_before, end_hook,
        )
    left = events[2 * parts :]
    heads_out[...] = filtered_grad[0:8, :]
    back_copy = remote(heads_out, following, halo_sem, 1, seq=q - 1)
    pl.when(jnp.logical_not(first))(back_copy.start)

    @pl.when(last)
    def _():
        following[...] = jnp.zeros_like(following)

    small[...] = filter_sums[...]
    small[count + 1 : count + 2, 0:inner] = norm_grad[0:1, :]
    for row in range(3):
        small[count + 2 : count + 3, row * LANES : (row + 1) * LANES] = head_sums[row : row + 1, :]

    steps = [("dp", bit) for bit in (1, 2)] + [("seq", bit) for bit in bits]

    def small_copy(number):
        axis, bit = steps[number]
        target = {"seq": toggled(q, bit)} if axis == "seq" else {"dp": toggled(d, bit)}
        return remote(small_in.at[2 * number], small_in.at[2 * number + 1], small_sem, number, **target)

    def small_start(number):
        small_in[2 * number] = small[...]
        small_copy(number).start()

    def small_step(number):
        with jax.named_scope("small_wait"):
            small_copy(number).wait()
        small[...] += small_in[2 * number + 1]
        if number + 1 < len(steps):
            small_start(number + 1)

    small_start(0)

    @pl.when(near)
    def _():
        for event in events[parts : 2 * parts]:
            weight_event(*event)

    small_step(0)
    pl.when(jnp.logical_not(last))(back_copy.wait_recv)
    with jax.named_scope("filter_grad"):
        filter_grad_phase(filtered_grad, following, taps, window, input_grad)
    small_step(1)
    for event in left[:parts]:
        weight_event(*event)
    left = left[parts:]
    number = 2
    while left or number < len(steps):
        for event in left[:parts]:
            weight_event(*event)
        left = left[parts:]
        for _ in range(2 if len(left) == parts else 1):
            if number < len(steps):
                small_step(number)
                number += 1

    store_weight = pltpu.make_async_copy(weight_all, weight_result, local_sem.at[1])
    store_weight.start()
    filter_out[...] = small[0 : count + 1, :]
    for index in range(inner // LANES):
        norm_out[index : index + 1, :] = small[
            count + 1 : count + 2, index * LANES : (index + 1) * LANES
        ]
    for row in range(3):
        head_out[row : row + 1, :] = small[
            count + 2 : count + 3, row * LANES : row * LANES + step.shape[0]
        ]
    for number in halvings:
        for part in range(parts):
            spread_copy(number, part).wait_send()
    gather(d, 0, across).wait_send()
    gather(d, 1, beside).wait_send()
    gather(across, 2, beside).wait_send()
    for slot in (1, 2, 3):
        partial_copy(slot).wait_send()
    for slot, peer in enumerate(peers):
        column_copy(slot, peer).wait_send()
    pl.when(jnp.logical_not(last))(halo_copy.wait_send)
    pl.when(jnp.logical_not(first))(back_copy.wait_send)

    def drain(index, carry):
        chain_end(index, states, states_other, entering, ahead_sems, ends, q + 2)
        chain_end(index, back_states, back_other, end_grad, back_sems, begins, q - 2)
        return carry

    with jax.named_scope("drain"):
        lax.fori_loop(0, messages, drain, 0)
    store_gate.wait()
    store_weight.wait()


def body(
    conv_input,
    gate_input,
    step_input,
    filter_taps,
    filter_bias,
    step_bias,
    decay_log,
    skip_gain,
    norm_weight,
    output_weight,
    output_grad,
):
    raw, gate, step, cotangent = conv_input[0], gate_input[0], step_input[0], output_grad[0]
    tokens, channels = raw.shape
    inner = gate.shape[1]
    heads = step.shape[0]
    own_rows, width = output_weight.shape
    count = filter_taps.shape[0]
    spans, groups = lax.axis_size("seq"), lax.axis_size("dp")
    half = tokens // 2
    chunks = inner // LANES
    messages = chunks // 2
    assert groups == 4 and tokens % 256 == 0 and inner % (2 * LANES) == 0
    levels = spans.bit_length() - 1
    shared, size = 0, own_rows
    for _ in range(levels):
        size = size // 2 if size // 2 % 16 == 0 else size
        shared += size
    wide = pltpu.VMEM((tokens, inner), F32)
    full = pltpu.VMEM((tokens, channels), F32)
    columns = pltpu.VMEM((tokens, LANES), F32)
    row8 = pltpu.VMEM((8, inner), F32)
    stored = pltpu.VMEM((chunks, LANES, LANES), F32)
    turned = pltpu.VMEM((2, LANES, tokens), BF16)
    squares = pltpu.VMEM((3, half, half), F32)
    edge = pltpu.VMEM((8, channels), F32)
    sems = pltpu.SemaphoreType.DMA
    scratch = [
        pltpu.VMEM((tokens, inner), BF16), pltpu.VMEM((tokens, inner), BF16),
        pltpu.VMEM((own_rows, width), F32), edge, row8,
        pltpu.VMEM((16, channels), BF16),
        pltpu.VMEM((own_rows, width), BF16),
        pltpu.VMEM((groups, tokens, width), BF16),
        full, full, wide, wide, row8, row8,
        pltpu.VMEM((heads, 1, tokens), F32), columns, columns, turned, turned,
        pltpu.VMEM((2, tokens + 8, LANES), F32), squares,
        stored, stored, stored, wide, wide, columns,
        pltpu.VMEM((groups, tokens, own_rows), BF16),
        pltpu.VMEM((groups, tokens, own_rows), BF16),
        pltpu.VMEM((groups, tokens, own_rows), F32),
        pltpu.VMEM((groups, tokens, own_rows), BF16),
        pltpu.VMEM((tokens, own_rows), F32),
        pltpu.VMEM((2, tokens, own_rows), BF16),
        wide, wide, row8, row8,
        stored, stored, stored, squares, columns, columns, columns,
        edge, pltpu.VMEM((8, LANES), F32), edge, edge,
        pltpu.VMEM((shared, width), BF16),
        pltpu.VMEM((shared, width), BF16),
        pltpu.VMEM((own_rows, width), BF16),
        pltpu.VMEM((2 * (levels + 2), 8, channels), F32),
        sems((3,)), sems((2, 2)), sems((2, 1)), sems((2, 3)), sems((2, 3)), sems((2, 3)),
        sems((2, messages)), sems((2, messages)), sems((2, 2, messages)), sems((2, 2, messages)),
        sems((2, 8 * levels)), sems((2, levels + 2)),
    ]
    outs = [
        ((tokens, channels), BF16), ((tokens, inner), BF16), ((heads, tokens), F32),
        ((own_rows, width), BF16), ((count + 1, channels), F32), ((chunks, LANES), F32),
        ((3, heads), F32),
    ]
    args = (
        raw, step, filter_taps, filter_bias.reshape(channels // LANES, LANES),
        step_bias[None], decay_log[None], skip_gain[None],
        norm_weight.reshape(chunks, LANES), output_weight, cotangent, gate,
    )
    vmem = pl.BlockSpec(memory_space=pltpu.VMEM)
    anywhere = pl.BlockSpec(memory_space=pl.ANY)
    results = pl.pallas_call(
        functools.partial(layer_kernel, spans, groups),
        out_shape=[jax.ShapeDtypeStruct(shape, kind) for shape, kind in outs],
        in_specs=[vmem] * (len(args) - 3) + [anywhere] * 3,
        out_specs=[vmem, anywhere, vmem, anywhere, vmem, vmem, vmem],
        scratch_shapes=scratch,
        compiler_params=pltpu.CompilerParams(
            vmem_limit_bytes=67043328, has_side_effects=True, collective_id=0
        ),
    )(*args)
    kinds = [outs[number] for number in range(len(outs))]
    kinds[3] = ((own_rows, width), F32)
    input_grad, gate_grad, step_grad, weight_grad, filter_grads, norm_grad, head_grads = pl.pallas_call(
        finish_kernel,
        out_shape=[jax.ShapeDtypeStruct(shape, kind) for shape, kind in kinds],
        in_specs=[anywhere] * len(outs),
        out_specs=[anywhere] * len(outs),
        scratch_shapes=[pltpu.VMEM(*out) for out in outs]
        + [pltpu.VMEM(*kinds[3]), sems((len(outs),)), sems((len(outs),))],
        compiler_params=pltpu.CompilerParams(vmem_limit_bytes=67043328),
    )(*results)
    return (
        input_grad[None], gate_grad[None], step_grad[None], weight_grad,
        filter_grads, norm_grad.reshape(inner), head_grads,
    )


def finish_kernel(*refs):
    count = (len(refs) - 3) // 3
    sources, targets, held = refs[:count], refs[count : 2 * count], list(refs[2 * count : 3 * count])
    widened, load_sem, store_sem = refs[3 * count :]
    loads = [
        pltpu.make_async_copy(source, buffer, load_sem.at[number])
        for number, (source, buffer) in enumerate(zip(sources, held))
    ]
    order = [3] + [number for number in range(count) if number != 3]
    for number in order:
        loads[number].start()
    stores = []
    for number in order:
        loads[number].wait()
        buffer = held[number]
        if number == 3:
            widened[...] = buffer[...].astype(F32)
            buffer = widened
        store = pltpu.make_async_copy(buffer, targets[number], store_sem.at[number])
        store.start()
        stores.append(store)
    for store in stores:
        store.wait()


def solution(mesh):
    return jax.shard_map(
        body,
        mesh=mesh,
        in_specs=(
            P("dp", "seq", None),
            P("dp", "seq", None),
            P("dp", None, "seq"),
            P(),
            P(),
            P(),
            P(),
            P(),
            P(),
            P("dp", None),
            P("dp", "seq", None),
        ),
        out_specs=(
            P("dp", "seq", None),
            P("dp", "seq", None),
            P("dp", None, "seq"),
            P("dp", None),
            P(),
            P(),
            P(),
        ),
        check_vma=False,
    )
```
